512 devices in a mesh: cuts: 4 (over z_hi), fsdp: 128 (over y, x, z_lo, core).
Axes of the slice: x: 4, y: 4, z: 16 (z_hi: 4, z_lo: 4; z = z_hi * 4 + z_lo), core: 2. Of those that a mesh axis runs over, the one named last changes fastest.
Arguments:
- tokens: bfloat16 [65536, 8192], P(('cuts', 'fsdp')), may hold values from -240 to 240
- norm_gain: bfloat16 [8192], P('fsdp'), may hold values from 0.5 to 1.5
- gate_weight: bfloat16 [8192, 256], P('fsdp'), may hold values from -0.0625 to 0.0625
- up_weight: bfloat16 [8192, 256], P('fsdp'), may hold values from -0.0625 to 0.0625
- down_weight: bfloat16 [256, 8192], P(None, 'fsdp'), may hold values from -0.375 to 0.375
- slice_grads: float32 [4, 3, 8192, 256], P('cuts', None, 'fsdp'), may hold values from -6 to 6
Outputs:
- branch_out: bfloat16 [65536, 8192], P(('cuts', 'fsdp'))
- grad_mean: float32 [3, 8192, 256], P(None, 'fsdp')
The draws below stay inside these ranges and needn't reach their ends.
All inputs are finite; a program needn't handle non-finite values.
Results may differ from the reference program's by a relative error of at most 0.0065.
Values may be sent and summed in bfloat16 or wider, within the bound.
A program may use at most 64 MiB of HBM per device.

```python
import math
import jax
import jax.numpy as jnp
from jax import lax

D = 8192
F = 256
TOK_DEV = 128
TOKENS = 65536
N_CUTS = 4


def draw_tokens(key, part):
    key_base = jax.random.fold_in(key, 11)
    key_rows = jax.random.fold_in(key, 12)
    key_cols = jax.random.fold_in(key, 13)
    base_draw = jax.random.normal(key_base, (TOKENS, D), jnp.float32)
    base_draw = jnp.clip(base_draw, -6.0, 6.0)
    row_scale = jnp.exp(jax.random.uniform(key_rows, (TOKENS, 1), jnp.float32, 0.0, math.log(10.0)))
    col_scale = jnp.exp(jax.random.uniform(key_cols, (1, D), jnp.float32, math.log(0.4), math.log(4.0)))
    return (base_draw * row_scale * col_scale).astype(jnp.bfloat16)


def levels(own_key, extent, cuts, low, high):
    def one(position, blocks):
        draws = jax.random.uniform(jax.random.fold_in(jax.random.fold_in(own_key, 6), position), (blocks,), jnp.float32, low / len(cuts), high / len(cuts))
        return jnp.repeat(jnp.exp(draws), extent[position] // blocks).reshape((-1,) + (1,) * (len(extent) - position - 1))

    loudness = one(*cuts[0])
    for cut in cuts[1:]:
        loudness = loudness * one(*cut)
    return loudness


def gaussian(key, shape, width, most, cuts=(), held_as=jnp.bfloat16):
    loudness = levels(key, shape, cuts, -0.22, 0.18) if cuts else 1.0
    values = jax.random.normal(key, shape, jnp.float32) * width * loudness
    return jnp.minimum(jnp.maximum(values, -most), most).astype(held_as)


def setup_inputs(seed: int = 0) -> dict:
    key_list = jax.random.split(jax.random.key(seed), 7)
    tokens = draw_tokens(jax.random.fold_in(key_list[6], 71), 0)
    norm_gain = jnp.clip(1.0 + 0.1 * jax.random.normal(key_list[1], (D,), jnp.float32), 0.5, 1.5).astype(jnp.bfloat16)
    gate_weight = gaussian(key_list[2], (D, F), D ** -0.5, 0.0625, ((0, 128),))
    up_weight = gaussian(key_list[3], (D, F), D ** -0.5, 0.0625, ((0, 128),))
    down_weight = gaussian(key_list[4], (F, D), F ** -0.5, 0.375, ((1, 128),))
    slice_grads = gaussian(key_list[5], (N_CUTS, 3, D, F), 1.0, 6.0, ((0, 4), (2, 128)), jnp.float32)
    return {"tokens": tokens, "norm_gain": norm_gain, "gate_weight": gate_weight, "up_weight": up_weight, "down_weight": down_weight, "slice_grads": slice_grads}


def feed_block(token_block, norm_gain, gate_weight, up_weight, down_weight):
    tok_float = token_block.astype(jnp.float32)
    inv_rms = lax.rsqrt(lax.optimization_barrier(jnp.mean(tok_float * tok_float, axis=1, keepdims=True)) + 1e-05)
    normed = (tok_float * inv_rms * norm_gain.astype(jnp.float32)[None, :]).astype(jnp.bfloat16)
    gate_out = jnp.dot(normed, gate_weight, preferred_element_type=jnp.float32)
    up_out = jnp.dot(normed, up_weight, preferred_element_type=jnp.float32)
    hidden = (jax.nn.silu(gate_out) * up_out).astype(jnp.bfloat16)
    return jnp.dot(hidden, down_weight, preferred_element_type=jnp.float32).astype(jnp.bfloat16)

def reference(tokens, norm_gain, gate_weight, up_weight, down_weight, slice_grads):
    block_rows = 4 * TOK_DEV
    blocked = tokens.reshape(TOKENS // block_rows, block_rows, D)

    def one_block(token_block):
        return feed_block(token_block, norm_gain, gate_weight, up_weight, down_weight)
    branch_out = lax.map(one_block, blocked).reshape(TOKENS, D)
    grad_mean = lax.optimization_barrier(jnp.sum(slice_grads, axis=0)) / N_CUTS
    return (branch_out, grad_mean)
```

```python
import jax
import jax.numpy as jnp
from jax import lax
from jax.experimental import pallas as pl
from jax.experimental.pallas import tpu as pltpu
from jax.sharding import Mesh
from jax.sharding import PartitionSpec as P

MESH = pl.DeviceIdType.MESH
FSDP = ("y", "x", "zl", "core")
CUTS_FSDP = ("cuts", "y", "x", "zl", "core")
ALL = slice(None)
NEAR = (0, -1, 1, 2)
F32 = jnp.float32
BF16 = jnp.bfloat16


class Numbers:
    def __init__(self):
        self.of = {}

    def __call__(self, *key):
        return self.of.setdefault(key, len(self.of))


def message_numbers():
    number = Numbers()
    for p in range(2):
        for d in range(2):
            number("t1", p, d)
            number("t4", p, d)
            number("z2", p, d)
            for j in NEAR:
                number("z1", p, d, j)
            for zr in NEAR:
                number("y2", p, d, zr)
                for j in NEAR:
                    number("y1", p, d, zr, j)
        for r in NEAR:
            for zr in NEAR:
                number("d2d", p, r, zr)
    for d in range(2):
        for name in ("rs1", "rs2", "ag1", "ag2"):
            number(name, d)
    return number


NUMBER = message_numbers()
N_MESSAGES = len(NUMBER.of)


def kernel(
    tok_hbm, gain_hbm, gate_hbm, up_hbm, down_hbm, grads_hbm,
    out, grad_out,
    buf_p, buf_q, tok, acc, hid, inv,
    gain_in, gate_in, up_in, down_in,
    grad_in, rs1, part, rs2,
    send_sem, recv_sem, in_sem,
):
    bufs = (buf_p, buf_q)
    h, y, x, zl, c = (lax.axis_index(a) for a in CUTS_FSDP)

    def ring(v, s, n=4):
        return lax.rem(v + (s + n), n)

    def neighbour(axis, s):
        if axis == "y":
            return {"y": ring(y, s)}
        if axis == "x":
            return {"x": ring(x, s)}
        if axis == "cut":
            return {"cuts": ring(h, s)}
        if axis == "core":
            return {"core": 1 - c}
        zz = lax.rem(h * 4 + zl + (s + 16), 16)
        return {"cuts": lax.div(zz, 4), "zl": lax.rem(zz, 4)}

    SIGN = (1, -1)
    BACK = (-1, 1)
    first = ("x", "y")
    last = ("y", "x")
    mine1 = (x, y)
    mine2 = (y, x)

    def shard(p, j, zr, r, half=None, core=None):
        i1 = ALL if j is ALL else ring(mine1[p], j)
        i2 = ring(mine2[p], r)
        yy, xx = (i2, i1) if p == 0 else (i1, i2)
        lanes = ALL if half is None else pl.ds(half * 128, 128)
        return bufs[p].at[yy, xx, ring(zl, zr), c if core is None else core, :, lanes]

    sent = []

    def copy_of(key, src, dst, axis, s):
        k = NUMBER.of[key]
        return pltpu.make_async_remote_copy(
            src_ref=src, dst_ref=dst, send_sem=send_sem.at[k], recv_sem=recv_sem.at[k],
            device_id=neighbour(axis, s), device_id_type=MESH,
        )

    def send(key, ref, axis, s, dst=None):
        copy = copy_of(key, ref, ref if dst is None else dst, axis, s)
        copy.start()
        sent.append(copy)

    def arrived(key, ref, axis, s):
        copy_of(key, ref, ref, axis, s).wait_recv()

    loads = [
        pltpu.make_async_copy(src, dst, in_sem.at[k])
        for k, (src, dst) in enumerate(
            (
                (gain_hbm, gain_in),
                (gate_hbm, gate_in),
                (down_hbm, down_in),
                (up_hbm, up_in),
                (grads_hbm.at[0], grad_in),
                (tok_hbm, tok),
            )
        )
    ]
    for load in loads:
        load.start()

    barrier = pltpu.get_barrier_semaphore()
    partners = [("cut", 1), ("cut", -1), ("x", 1), ("x", -1), ("y", 1), ("y", -1), ("z", 1), ("z", -1), ("core", 1)]
    for axis, s in partners:
        pl.semaphore_signal(barrier, inc=1, device_id=neighbour(axis, s), device_id_type=MESH)

    loads[0].wait()
    rows = lax.broadcasted_iota(jnp.int32, (64, 64), 0)
    cols = lax.broadcasted_iota(jnp.int32, (64, 64), 1)
    gain_row = jnp.broadcast_to(gain_in[...].astype(F32), (64, 64))
    gain = jnp.sum(jnp.where(rows == cols, gain_row, 0.0), axis=1, keepdims=True)
    loads[1].wait()
    buf_p[y, x, zl, c, 0:64, :] = (gate_in[...].astype(F32) * gain).astype(BF16)
    loads[2].wait()
    buf_p[y, x, zl, c, 64:96, :] = down_in[0:32]
    buf_q[y, x, zl, c, 64:96, :] = down_in[32:64]
    loads[3].wait()
    buf_q[y, x, zl, c, 0:64, :] = (up_in[...].astype(F32) * gain).astype(BF16)
    loads[4].wait()

    pl.semaphore_wait(barrier, len(partners))

    def quarter(ref, q, half=None):
        lanes = ALL if half is None else pl.ds(half * 128, 128)
        return ref.at[:, pl.ds(pl.multiple_of(q * 16, 16), 16), lanes]

    BOTH = [(p, d) for d in range(2) for p in range(2)]

    for p, d in BOTH:
        send(("t1", p, d), shard(p, 0, 0, 0), first[p], SIGN[d])
    for d in range(2):
        send(("rs1", d), quarter(grad_in, ring(h, 2), d), "cut", SIGN[d], rs1.at[d])
    for p, d in BOTH:
        send(("z1", p, d, 0), shard(p, 0, 0, 0), "z", SIGN[d])
    for p, d in BOTH:
        send(("y1", p, d, 0, 0), shard(p, 0, 0, 0), last[p], SIGN[d])

    loads[5].wait()

    def square(k, total):
        v = tok[:, pl.ds(pl.multiple_of(k * 128, 128), 128)].astype(F32)
        return total + v * v

    total = lax.fori_loop(0, 64, square, jnp.zeros((128, 128), F32), unroll=4)
    mean = jnp.sum(total, axis=1, keepdims=True) * (1.0 / 8192.0)
    inv[...] = jnp.broadcast_to(lax.rsqrt(mean + 1e-5), (128, 128))
    acc[...] = jnp.zeros_like(acc)

    for p, d in BOTH:
        j = BACK[d]
        arrived(("t1", p, d), shard(p, j, 0, 0), first[p], SIGN[d])
        send(("t4", p, d), shard(p, j, 0, 0, d), first[p], SIGN[d])
        for e in range(2):
            send(("z1", p, e, j), shard(p, j, 0, 0), "z", SIGN[e])
        for e in range(2):
            send(("y1", p, e, 0, j), shard(p, j, 0, 0), last[p], SIGN[e])
    for p, d in BOTH:
        zr = BACK[d]
        arrived(("z1", p, d, 0), shard(p, 0, zr, 0), "z", SIGN[d])
        for e in range(2):
            send(("y1", p, e, zr, 0), shard(p, 0, zr, 0), last[p], SIGN[e])
    for p in range(2):
        for d in range(2):
            arrived(("t4", p, d), shard(p, 2, 0, 0, d), first[p], SIGN[d])
        for e in range(2):
            send(("z1", p, e, 2), shard(p, 2, 0, 0), "z", SIGN[e])
        for e in range(2):
            send(("y1", p, e, 0, 2), shard(p, 2, 0, 0), last[p], SIGN[e])
        send(("d2d", p, 0, 0), shard(p, ALL, 0, 0), "core", 1)

    for d in range(2):
        arrived(("rs1", d), rs1.at[d], "cut", SIGN[d])
        q = pl.ds(pl.multiple_of(ring(h, SIGN[d]) * 16, 16), 16)
        part[d] = grad_in[:, q, :]
        lanes = pl.ds(d * 128, 128)
        part[d, :, :, lanes] = grad_in[:, q, lanes] + rs1[d]

    for j in (-1, 1):
        for p, d in BOTH:
            zr = BACK[d]
            arrived(("z1", p, d, j), shard(p, j, zr, 0), "z", SIGN[d])
            for e in range(2):
                send(("y1", p, e, zr, j), shard(p, j, zr, 0), last[p], SIGN[e])
        if j == -1:
            for d in range(2):
                send(("rs2", d), part.at[d], "cut", SIGN[d], rs2.at[d])
    for p, d in BOTH:
        zr = BACK[d]
        arrived(("z1", p, d, 2), shard(p, 2, zr, 0), "z", SIGN[d])
        send(("z2", p, d), shard(p, ALL, zr, 0, d), "z", SIGN[d])
        for e in range(2):
            send(("y1", p, e, zr, 2), shard(p, 2, zr, 0), last[p], SIGN[e])
        send(("d2d", p, 0, zr), shard(p, ALL, zr, 0), "core", 1)

    def last_axis(zr, js):
        for p, d in BOTH:
            r = BACK[d]
            for j in js:
                arrived(("y1", p, d, zr, 0 if j is ALL else j), shard(p, j, zr, r), last[p], SIGN[d])
            send(("y2", p, d, zr), shard(p, ALL, zr, r, d), last[p], SIGN[d])
            send(("d2d", p, r, zr), shard(p, ALL, zr, r), "core", 1)

    def far_plane(zr):
        for p in range(2):
            for d in range(2):
                arrived(("y2", p, d, zr), shard(p, ALL, zr, 2, d), last[p], SIGN[d])
            send(("d2d", p, 2, zr), shard(p, ALL, zr, 2), "core", 1)

    def multiply(r):
        for p in range(2):
            for zr in NEAR:
                arrived(("d2d", p, r, zr), shard(p, ALL, zr, r, core=1 - c), "core", 1)
            i2 = ring(mine2[p], r)
            n = pl.ds(p * 256, 256)

            def step(k, _, p=p, i2=i2, n=n):
                yy, xx = (i2, k) if p == 0 else (k, i2)
                w = bufs[p][yy, xx, :, :, 0:64, :].reshape(512, 256)
                t = tok[:, pl.ds(pl.multiple_of((yy * 4 + xx) * 512, 512), 512)]
                acc[:, n] += jnp.dot(t, w, preferred_element_type=F32)
                return 0

            lax.fori_loop(0, 4, step, 0)

    last_axis(0, NEAR)
    for p in range(2):
        for d in range(2):
            arrived(("z2", p, d), shard(p, ALL, 2, 0, d), "z", SIGN[d])
        for e in range(2):
            send(("y1", p, e, 2, 0), shard(p, ALL, 2, 0), last[p], SIGN[e])
        send(("d2d", p, 0, 2), shard(p, ALL, 2, 0), "core", 1)

    q = pl.ds(pl.multiple_of(h * 16, 16), 16)
    for d in range(2):
        arrived(("rs2", d), rs2.at[d], "cut", SIGN[d])
    grad_out[:, q, :] = (grad_in[:, q, :] + rs2[0] + rs2[1]) * 0.25

    last_axis(-1, NEAR)
    for d in range(2):
        send(("ag1", d), quarter(grad_out, h), "cut", SIGN[d])
    last_axis(1, NEAR)
    multiply(0)
    far_plane(0)
    last_axis(2, (ALL,))
    far_plane(-1)
    for d in range(2):
        arrived(("ag1", d), quarter(grad_out, ring(h, BACK[d])), "cut", SIGN[d])
        send(("ag2", d), quarter(grad_out, ring(h, BACK[d]), d), "cut", SIGN[d])
    multiply(-1)
    far_plane(1)
    multiply(1)
    far_plane(2)
    for d in range(2):
        arrived(("ag2", d), quarter(grad_out, ring(h, 2), d), "cut", SIGN[d])
    multiply(2)

    gate = acc[:, 0:256] * inv[:, 0:1]
    up = acc[:, 256:512] * inv[:, 0:1]
    hid[...] = (gate / (1.0 + jnp.exp(-gate)) * up).astype(BF16)

    def project(k, _):
        yy, xx = lax.div(k, 4), lax.rem(k, 4)
        w = jnp.concatenate([b[yy, xx, :, :, 64:96, :] for b in bufs], axis=2).reshape(512, 256)
        block = lax.dot_general(hid[...], w, (((1,), (1,)), ((), ())), preferred_element_type=F32)
        out[:, pl.ds(pl.multiple_of(k * 512, 512), 512)] = block.astype(BF16)
        return 0

    lax.fori_loop(0, 16, project, 0)

    for copy in sent:
        copy.wait_send()


def per_device(tokens, norm_gain, gate_weight, up_weight, down_weight, slice_grads):
    hbm = pl.BlockSpec(memory_space=pltpu.HBM)
    vmem = pl.BlockSpec(memory_space=pltpu.VMEM)
    return pl.pallas_call(
        kernel,
        out_shape=(
            jax.ShapeDtypeStruct(tokens.shape, BF16),
            jax.ShapeDtypeStruct(slice_grads.shape[1:], F32),
        ),
        in_specs=[hbm] * 6,
        out_specs=(vmem, vmem),
        scratch_shapes=[
            pltpu.VMEM((4, 4, 4, 2, 96, 256), BF16),
            pltpu.VMEM((4, 4, 4, 2, 96, 256), BF16),
            pltpu.VMEM((128, 8192), BF16),
            pltpu.VMEM((128, 512), F32),
            pltpu.VMEM((128, 256), BF16),
            pltpu.VMEM((128, 128), F32),
            pltpu.VMEM((1, 64), BF16),
            pltpu.VMEM((64, 256), BF16),
            pltpu.VMEM((64, 256), BF16),
            pltpu.VMEM((64, 256), BF16),
            pltpu.VMEM((3, 64, 256), F32),
            pltpu.VMEM((2, 3, 16, 128), F32),
            pltpu.VMEM((2, 3, 16, 256), F32),
            pltpu.VMEM((2, 3, 16, 256), F32),
            pltpu.SemaphoreType.DMA((N_MESSAGES,)),
            pltpu.SemaphoreType.DMA((N_MESSAGES,)),
            pltpu.SemaphoreType.DMA((6,)),
        ],
        compiler_params=pltpu.CompilerParams(
            collective_id=0, has_side_effects=True, vmem_limit_bytes=67043328
        ),
    )(tokens, norm_gain.reshape(1, 64), gate_weight, up_weight, down_weight.T, slice_grads)


def solution(mesh):
    finer = Mesh(mesh.devices.reshape(mesh.shape["cuts"], 4, 4, 4, 2), CUTS_FSDP)
    in_specs = (
        P(CUTS_FSDP, None),
        P(FSDP),
        P(FSDP, None),
        P(FSDP, None),
        P(None, FSDP),
        P("cuts", None, FSDP, None),
    )
    out_specs = (P(CUTS_FSDP, None), P(None, FSDP, None))
    return jax.shard_map(
        per_device, mesh=finer, in_specs=in_specs, out_specs=out_specs, check_vma=False
    )
```

```python
import jax
import jax.numpy as jnp
from jax import lax
from jax.experimental import pallas as pl
from jax.experimental.pallas import tpu as pltpu
from jax.sharding import Mesh
from jax.sharding import PartitionSpec as P

MESH = pl.DeviceIdType.MESH
FSDP = ("y", "x", "zl", "core")
CUTS_FSDP = ("cuts", "y", "x", "zl", "core")
ALL = slice(None)
NEAR = (0, -1, 1, 2)
F32 = jnp.float32
BF16 = jnp.bfloat16


PARTS = range(2)
WAYS = range(2)

RECV = [("t1", p, d) for p in PARTS for d in WAYS]
RECV += [("t4", p) for p in PARTS] + [("z2", p) for p in PARTS] + [("c0", p) for p in PARTS]
RECV += [("z1", p, d, j) for p in PARTS for d in WAYS for j in NEAR]
RECV += [("g1", p, d, zr) for p in PARTS for d in WAYS for zr in NEAR]
RECV += [("g2", p, zr) for p in PARTS for zr in NEAR]
RECV += [("d1", p, d, zr) for p in PARTS for d in WAYS for zr in NEAR[1:]]
RECV += [("d2", p, zr) for p in PARTS for zr in NEAR[1:]]
RECV += [(name, p, r) for name in ("cg", "cd") for p in PARTS for r in (-1, 1, 2)]
GRADS = [(name, d) for name in ("rs1", "rs2", "ag1", "ag2") for d in WAYS]
RECV = {key: k for k, key in enumerate(RECV + GRADS)}
KINDS = ("t1", "t4", "z1", "z2", "g1", "g2", "d1", "d2", "c0", "cg", "cd")
SENT = {key: k for k, key in enumerate([(kind, p) for kind in KINDS for p in PARTS] + GRADS)}


def kernel(
    tok_hbm, gain_hbm, gate_hbm, up_hbm, down_hbm, grads_hbm,
    out, grad_out,
    buf_p, buf_q, tok, acc, hid, inv,
    gain_in, gate_in, up_in, down_in,
    grad_in, rs1, part, rs2, mean_out,
    send_sem, recv_sem, in_sem, here,
):
    bufs = (buf_p, buf_q)
    h, y, x, zl, c = (lax.axis_index(a) for a in CUTS_FSDP)

    def ring(v, s, n=4):
        return lax.rem(v + (s + n), n)

    def neighbour(axis, s):
        if axis == "y":
            return {"y": ring(y, s)}
        if axis == "x":
            return {"x": ring(x, s)}
        if axis == "cut":
            return {"cuts": ring(h, s)}
        if axis == "core":
            return {"core": 1 - c}
        zz = lax.rem(h * 4 + zl + (s + 16), 16)
        return {"cuts": lax.div(zz, 4), "zl": lax.rem(zz, 4)}

    SIGN = (1, -1)
    BACK = (-1, 1)
    first = ("x", "y")
    last = ("y", "x")
    mine1 = (x, y)
    mine2 = (y, x)

    GATED, DOWN = pl.ds(0, 64), pl.ds(64, 32)

    def shard(p, j, zr, r, half=None, rows=ALL, core=None):
        i1 = ALL if j is ALL else ring(mine1[p], j)
        iz = ALL if zr is ALL else ring(zl, zr)
        i2 = ring(mine2[p], r)
        yy, xx = (i2, i1) if p == 0 else (i1, i2)
        lanes = ALL if half is None else pl.ds(half * 128, 128)
        return bufs[p].at[yy, xx, iz, c if core is None else core, rows, lanes]

    def copy_of(key, src, dst, axis, s):
        return pltpu.make_async_remote_copy(
            src_ref=src,
            dst_ref=dst,
            send_sem=send_sem.at[SENT[key if key in GRADS else key[:2]]],
            recv_sem=recv_sem.at[RECV[key]],
            device_id=neighbour(axis, s),
            device_id_type=MESH,
        )

    def give(key, axis, s, *where, **also):
        ref = shard(*where, **also)
        copy_of(key, ref, ref, axis, s).start()

    def arrived(key, ref):
        copy_of(key, ref, ref, "core", 1).wait_recv()

    def taken(key, *where, **also):
        arrived(key, shard(*where, **also))

    def all_sent():
        for p in PARTS:
            b = bufs[p]
            for kind, ref in (
                ("t1", b.at[0, 0, 0]),
                ("t4", b.at[0, 0, 0, 0]),
                ("z1", b.at[0, 0]),
                ("g1", b.at[0, 0:3]),
                ("g2", b.at[0, 0:3, 0:2]),
                ("d1", b.at[0, 0]),
                ("d2", b.at[0, 0, 0:2]),
                ("c0", b.at[0, 0:2]),
                ("cg", b.at[0:3, 0:2, :, :, 0:64]),
                ("cd", b.at[0:3, 0:2, :, :, 64:96]),
            ):
                pltpu.make_async_remote_copy(
                    src_ref=ref,
                    dst_ref=ref,
                    send_sem=send_sem.at[SENT[kind, p]],
                    recv_sem=recv_sem.at[0],
                    device_id=neighbour("core", 1),
                    device_id_type=MESH,
                ).wait_send()

            def second(ref):
                copy_of(("z2", p), ref, ref, "core", 1).wait_send()

            @pl.when(jnp.logical_or(zg == 0, zg == 15))
            def _():
                second(b.at[0, 0, 0])

            @pl.when(jnp.logical_or(zg == 1, zg == 2))
            def _():
                second(b.at[0, 0:3, 0])

            @pl.when(jnp.logical_and(zg > 2, zg < 15))
            def _():
                second(b.at[0, 0, 0:2])

        for d in WAYS:
            for name, ref in (("rs1", rs1.at[d]), ("rs2", rs2.at[d]), ("ag1", mean_out.at[0]), ("ag2", mean_out.at[0, :, :, 0:128])):
                copy_of((name, d), ref, ref, "core", 1).wait_send()

    def tell(k, s):
        pl.semaphore_signal(here.at[k], inc=1, device_id=neighbour("z", s), device_id_type=MESH)

    def told(k):
        pl.semaphore_wait(here.at[k], 1)

    zg = h * 4 + zl

    loads = [
        pltpu.make_async_copy(src, dst, in_sem.at[k])
        for k, (src, dst) in enumerate(
            (
                (gain_hbm, gain_in),
                (gate_hbm, gate_in),
                (down_hbm, down_in),
                (up_hbm, up_in),
                (grads_hbm.at[0], grad_in),
                (tok_hbm, tok),
            )
        )
    ]
    for load in loads:
        load.start()

    barrier = pltpu.get_barrier_semaphore()
    partners = [("x", 1), ("x", -1), ("y", 1), ("y", -1), ("z", -1), ("core", 1)]
    for axis, s in partners:
        pl.semaphore_signal(barrier, inc=1, device_id=neighbour(axis, s), device_id_type=MESH)

    loads[0].wait()
    rows = lax.broadcasted_iota(jnp.int32, (64, 64), 0)
    cols = lax.broadcasted_iota(jnp.int32, (64, 64), 1)
    gain_row = jnp.broadcast_to(gain_in[...].astype(F32), (64, 64))
    gain = jnp.sum(jnp.where(rows == cols, gain_row, 0.0), axis=1, keepdims=True)
    loads[1].wait()
    buf_p[y, x, zl, c, 0:64, :] = (gate_in[...].astype(F32) * gain).astype(BF16)
    loads[2].wait()
    buf_p[y, x, zl, c, 64:96, :] = down_in[0:32]
    buf_q[y, x, zl, c, 64:96, :] = down_in[32:64]
    loads[3].wait()
    buf_q[y, x, zl, c, 0:64, :] = (up_in[...].astype(F32) * gain).astype(BF16)

    pl.semaphore_wait(barrier, len(partners))

    def quarter(ref, q, half=None):
        lanes = ALL if half is None else pl.ds(half * 128, 128)
        return ref.at[:, pl.ds(pl.multiple_of(q * 16, 16), 16), lanes]

    BOTH = [(p, d) for d in WAYS for p in PARTS]

    def along_z(p, j):
        give(("z1", p, 0, j), "z", 1, p, j, 0, 0)

        @pl.when(zg > 0)
        def _():
            give(("z1", p, 1, j), "z", -1, p, j, 0, 0)

    def along_last(p, zr, j):
        for e in WAYS:
            give(("g1", p, e, zr), last[p], SIGN[e], p, j, zr, 0, rows=ALL if zr == 0 else GATED)

    for p, d in BOTH:
        give(("t1", p, d), first[p], SIGN[d], p, 0, 0, 0)
    tell(0, 1)
    for p in PARTS:
        give(("z1", p, 0, 0), "z", 1, p, 0, 0, 0)
    for p in PARTS:
        along_last(p, 0, 0)

    def below():
        told(0)
        tell(1, -1)
        tell(2, 1)

    def four_away():
        tell(3, -2)
        tell(4, 2)

    def exchange(d):
        src = quarter(grad_in, ring(h, 2), d)
        copy_of(("rs1", d), src, rs1.at[d], "cut", SIGN[d]).start()

    @pl.when(zg > 0)
    def _():
        below()
        for p in PARTS:
            give(("z1", p, 1, 0), "z", -1, p, 0, 0, 0)

    loads[4].wait()
    loads[5].wait()

    def square(k, total):
        v = tok[:, pl.ds(pl.multiple_of(k * 128, 128), 128)].astype(F32)
        return total + v * v

    total = lax.fori_loop(0, 64, square, jnp.zeros((128, 128), F32), unroll=4)
    mean = jnp.sum(total, axis=1, keepdims=True) * (1.0 / 8192.0)
    inv[...] = jnp.broadcast_to(lax.rsqrt(mean + 1e-5), (128, 128))
    acc[...] = jnp.zeros_like(acc)

    @pl.when(zg < 15)
    def _():
        told(1)

    @pl.when(zg > 1)
    def _():
        told(2)

    @pl.when(jnp.logical_and(zg > 1, zg < 15))
    def _():
        four_away()

    @pl.when(zg == 15)
    def _():
        told(1)
        four_away()

    @pl.when(zg < 13)
    def _():
        told(3)
        exchange(0)

    @pl.when(zg > 3)
    def _():
        told(4)
        exchange(1)

    def first_axis(p, d):
        j = BACK[d]
        taken(("t1", p, d), p, j, 0, 0)
        give(("t4", p), first[p], SIGN[d], p, j, 0, 0, half=d)
        along_z(p, j)
        along_last(p, 0, j)

    for p, d in BOTH:
        first_axis(p, d)

    def onward(p, d, j, half=True):
        give(("z2", p), "z", SIGN[d], p, j, BACK[d], 0, half=d if half else None)

    def from_z(d, js):
        zr = BACK[d]
        for j in js:
            for p in PARTS:
                taken(("z1", p, d, j), p, j, zr, 0)
                if d == 0:

                    @pl.when(jnp.logical_and(zg > 0, zg < 15))
                    def _():
                        onward(p, d, j)

                else:

                    @pl.when(zg > 2)
                    def _():
                        onward(p, d, j)

                    @pl.when(jnp.logical_or(zg == 1, zg == 2))
                    def _():
                        onward(p, d, j, half=False)

                along_last(p, zr, j)
        if js[-1] == 2:
            for p in PARTS:
                give(("c0", p), "core", 1, p, ALL, zr, 0)

    def first_far(p):
        taken(("t4", p), p, 2, 0, 0)
        along_z(p, 2)
        along_last(p, 0, 2)
        give(("c0", p), "core", 1, p, ALL, 0, 0)

    def down_near(zr):
        for p, d in BOTH:
            give(("d1", p, d, zr), last[p], SIGN[d], p, ALL, zr, 0, rows=DOWN)

    def gated_near(zr):
        for p, d in BOTH:
            r = BACK[d]
            rows = ALL if zr == 0 else GATED
            taken(("g1", p, d, zr), p, ALL, zr, r, rows=rows)
            give(("g2", p, zr), last[p], SIGN[d], p, ALL, zr, r, half=d, rows=rows)
            give(("cg", p, r), "core", 1, p, ALL, zr, r, rows=GATED)
            if zr == 0:
                give(("cd", p, r), "core", 1, p, ALL, zr, r, rows=DOWN)

    def gated_far(zr):
        for p in PARTS:
            taken(("g2", p, zr), p, ALL, zr, 2, rows=ALL if zr == 0 else GATED)
            give(("cg", p, 2), "core", 1, p, ALL, zr, 2, rows=GATED)
            if zr == 0:
                give(("cd", p, 2), "core", 1, p, ALL, zr, 2, rows=DOWN)

    def down_next(zr):
        for p, d in BOTH:
            r = BACK[d]
            taken(("d1", p, d, zr), p, ALL, zr, r, rows=DOWN)
            give(("d2", p, zr), last[p], SIGN[d], p, ALL, zr, r, half=d, rows=DOWN)
            give(("cd", p, r), "core", 1, p, ALL, zr, r, rows=DOWN)

    def down_far(zr):
        for p in PARTS:
            taken(("d2", p, zr), p, ALL, zr, 2, rows=DOWN)
            give(("cd", p, 2), "core", 1, p, ALL, zr, 2, rows=DOWN)

    def across_z():
        for p in PARTS:
            taken(("z2", p), p, ALL, 2, 0)
            along_last(p, 2, ALL)
            give(("c0", p), "core", 1, p, ALL, 2, 0)

    def multiply(r):
        for p in PARTS:
            if r == 0:
                taken(("c0", p), p, ALL, ALL, 0, core=1 - c)
            else:
                taken(("cg", p, r), p, ALL, ALL, r, rows=GATED, core=1 - c)
            i2 = ring(mine2[p], r)
            n = pl.ds(p * 256, 256)
            total = acc[:, n]
            for k in range(4):
                yy, xx = (i2, k) if p == 0 else (k, i2)
                w = bufs[p][yy, xx, :, :, 0:64, :].reshape(512, 256)
                t = tok[:, pl.ds(pl.multiple_of((yy * 4 + xx) * 512, 512), 512)]
                total = total + jnp.dot(t, w, preferred_element_type=F32)
            acc[:, n] = total

    def grads_partial():
        for d in WAYS:
            arrived(("rs1", d), rs1.at[d])
            q = pl.ds(pl.multiple_of(ring(h, SIGN[d]) * 16, 16), 16)
            part[d] = grad_in[:, q, :]
            lanes = pl.ds(d * 128, 128)
            part[d, :, :, lanes] = grad_in[:, q, lanes] + rs1[d]

    def grads_send():
        for d in WAYS:
            copy_of(("rs2", d), part.at[d], rs2.at[d], "cut", SIGN[d]).start()

    def grads_own():
        q = pl.ds(pl.multiple_of(h * 16, 16), 16)
        for d in WAYS:
            arrived(("rs2", d), rs2.at[d])
        mean_out[h] = ((grad_in[:, q, :] + rs2[0] + rs2[1]) * 0.25).astype(BF16)

    def grads_give():
        for d in WAYS:
            copy_of(("ag1", d), mean_out.at[h], mean_out.at[h], "cut", SIGN[d]).start()

    def grads_next():
        for d in WAYS:
            arrived(("ag1", d), mean_out.at[ring(h, BACK[d])])
            half = mean_out.at[ring(h, BACK[d]), :, :, pl.ds(d * 128, 128)]
            copy_of(("ag2", d), half, half, "cut", SIGN[d]).start()

    first_far(0)
    first_far(1)
    from_z(1, (0,))

    @pl.when(zg > 0)
    def _():
        from_z(0, (0,))

    @pl.when(zg == 0)
    def _():
        below()
        for p in PARTS:
            for j in NEAR:
                give(("z1", p, 1, j), "z", -1, p, j, 0, 0)
            onward(p, 1, 0)

    @pl.when(zg < 2)
    def _():
        told(2)
        four_away()

    gated_near(0)
    from_z(1, (-1, 1, 2))

    @pl.when(zg == 0)
    def _():
        for p in PARTS:
            for j in NEAR[1:]:
                onward(p, 1, j)

    down_near(1)

    @pl.when(zg > 12)
    def _():
        told(3)
        exchange(0)

    @pl.when(zg < 4)
    def _():
        told(4)
        exchange(1)

    grads_partial()
    grads_send()

    @pl.when(zg < 2)
    def _():
        gated_near(1)
        down_next(1)

    @pl.when(zg == 0)
    def _():
        from_z(0, (0,))

    from_z(0, (-1, 1, 2))
    down_near(-1)

    @pl.when(zg > 1)
    def _():
        gated_near(1)
        down_next(1)

    gated_near(-1)
    across_z()
    down_near(2)
    down_next(-1)
    grads_own()
    grads_give()
    gated_near(2)
    grads_next()
    down_next(2)
    gated_far(0)
    gated_far(1)
    multiply(0)
    gated_far(-1)
    multiply(-1)
    gated_far(2)
    multiply(1)
    down_far(1)
    down_far(-1)
    multiply(2)

    gate = acc[:, 0:256] * inv[:, 0:1]
    up = acc[:, 256:512] * inv[:, 0:1]
    hid[...] = (gate / (1.0 + jnp.exp(-gate)) * up).astype(BF16)

    def project(yy, xx):
        w = jnp.concatenate([b[yy, xx, :, :, 64:96, :] for b in bufs], axis=2).reshape(512, 256)
        block = lax.dot_general(hid[...], w, (((1,), (1,)), ((), ())), preferred_element_type=F32)
        out[:, pl.ds(pl.multiple_of((yy * 4 + xx) * 512, 512), 512)] = block.astype(BF16)

    for p in PARTS:
        for r in (-1, 1):
            taken(("cd", p, r), p, ALL, ALL, r, rows=DOWN, core=1 - c)

    def near(k, _):
        for i in range(3):
            project(ring(y, k - 1), ring(x, i - 1))
        return 0

    def last_part():
        for p in PARTS:
            taken(("cd", p, 2), p, ALL, ALL, 2, rows=DOWN, core=1 - c)
        for k in range(4):
            project(ring(y, 2), k)
        for k in range(3):
            project(ring(y, k - 1), ring(x, 2))

    def finish():
        for d in WAYS:
            arrived(("ag2", d), mean_out.at[ring(h, 2), :, :, pl.ds(d * 128, 128)])
        for k in range(4):
            grad_out[:, k * 16 : k * 16 + 16, :] = mean_out[k].astype(F32)

    down_far(2)
    lax.fori_loop(0, 3, near, 0)
    finish()
    last_part()
    all_sent()


def per_device(tokens, norm_gain, gate_weight, up_weight, down_weight, slice_grads):
    hbm = pl.BlockSpec(memory_space=pltpu.HBM)
    vmem = pl.BlockSpec(memory_space=pltpu.VMEM)
    return pl.pallas_call(
        kernel,
        out_shape=(
            pltpu.VMEM(tokens.shape, BF16),
            pltpu.VMEM(slice_grads.shape[1:], F32),
        ),
        in_specs=[hbm] * 6,
        out_specs=(vmem, vmem),
        scratch_shapes=[
            pltpu.VMEM((4, 4, 4, 2, 96, 256), BF16),
            pltpu.VMEM((4, 4, 4, 2, 96, 256), BF16),
            pltpu.VMEM((128, 8192), BF16),
            pltpu.VMEM((128, 512), F32),
            pltpu.VMEM((128, 256), BF16),
            pltpu.VMEM((128, 128), F32),
            pltpu.VMEM((1, 64), BF16),
            pltpu.VMEM((64, 256), BF16),
            pltpu.VMEM((64, 256), BF16),
            pltpu.VMEM((64, 256), BF16),
            pltpu.VMEM((3, 64, 256), F32),
            pltpu.VMEM((2, 3, 16, 128), F32),
            pltpu.VMEM((2, 3, 16, 256), F32),
            pltpu.VMEM((2, 3, 16, 256), F32),
            pltpu.VMEM((4, 3, 16, 256), BF16),
            pltpu.SemaphoreType.DMA((len(SENT),)),
            pltpu.SemaphoreType.DMA((len(RECV),)),
            pltpu.SemaphoreType.DMA((6,)),
            pltpu.SemaphoreType.REGULAR((5,)),
        ],
        compiler_params=pltpu.CompilerParams(
            collective_id=0, has_side_effects=True, vmem_limit_bytes=60000000
        ),
    )(tokens, norm_gain.reshape(1, 64), gate_weight, up_weight, down_weight.T, slice_grads)


def solution(mesh):
    finer = Mesh(mesh.devices.reshape(mesh.shape["cuts"], 4, 4, 4, 2), CUTS_FSDP)
    in_specs = (
        P(CUTS_FSDP, None),
        P(FSDP),
        P(FSDP, None),
        P(FSDP, None),
        P(None, FSDP),
        P("cuts", None, FSDP, None),
    )
    out_specs = (P(CUTS_FSDP, None), P(None, FSDP, None))
    return jax.shard_map(
        per_device, mesh=finer, in_specs=in_specs, out_specs=out_specs, check_vma=False
    )
```

```python
import jax
import jax.numpy as jnp
from jax import lax
from jax.experimental import pallas as pl
from jax.experimental.pallas import tpu as pltpu
from jax.sharding import Mesh
from jax.sharding import PartitionSpec as P

MESH = pl.DeviceIdType.MESH
FSDP = ("y", "x", "zl", "core")
CUTS_FSDP = ("cuts", "y", "x", "zl", "core")
ALL = slice(None)
NEAR = (0, -1, 1, 2)
F32 = jnp.float32
BF16 = jnp.bfloat16


PARTS = range(2)
WAYS = range(2)

RECV = [("t1", p, d) for p in PARTS for d in WAYS]
RECV += [("t4", p) for p in PARTS] + [("z2", p) for p in PARTS] + [("c0", p) for p in PARTS]
RECV += [("z1", p, d, j) for p in PARTS for d in WAYS for j in NEAR]
RECV += [("g1", p, d, zr) for p in PARTS for d in WAYS for zr in NEAR[1:]]
RECV += [("g1", p, d, 0, j) for p in PARTS for d in WAYS for j in NEAR]
RECV += [("g2", p, zr) for p in PARTS for zr in NEAR]
RECV += [("d1", p, d, zr) for p in PARTS for d in WAYS for zr in NEAR[1:]]
RECV += [("d2", p, zr) for p in PARTS for zr in NEAR[1:]]
RECV += [(name, p, r) for name in ("cg", "cd") for p in PARTS for r in (-1, 1, 2)]
GRADS = [(name, d) for name in ("rs1", "rs2", "ag1", "ag2") for d in WAYS]
RECV = {key: k for k, key in enumerate(RECV + GRADS)}
KINDS = ("t1", "t4", "z1", "z2", "g1", "g2", "d1", "d2", "c0", "cg", "cd")
SENT = {key: k for k, key in enumerate([(kind, p) for kind in KINDS for p in PARTS] + GRADS)}


def kernel(
    tok_hbm, gain_hbm, gate_hbm, up_hbm, down_hbm, grads_hbm,
    out, grad_out,
    buf_p, buf_q, tok, acc, hid, inv,
    gain_in, gate_in, up_in, down_in,
    grad_in, rs1, part, rs2, mean_out,
    send_sem, recv_sem, in_sem, here,
):
    bufs = (buf_p, buf_q)
    h, y, x, zl, c = (lax.axis_index(a) for a in CUTS_FSDP)

    def ring(v, s, n=4):
        return lax.rem(v + (s + n), n)

    def neighbour(axis, s):
        if axis == "y":
            return {"y": ring(y, s)}
        if axis == "x":
            return {"x": ring(x, s)}
        if axis == "cut":
            return {"cuts": ring(h, s)}
        if axis == "core":
            return {"core": 1 - c}
        zz = lax.rem(h * 4 + zl + (s + 16), 16)
        return {"cuts": lax.div(zz, 4), "zl": lax.rem(zz, 4)}

    SIGN = (1, -1)
    BACK = (-1, 1)
    first = ("x", "y")
    last = ("y", "x")
    mine1 = (x, y)
    mine2 = (y, x)

    GATED, DOWN = pl.ds(0, 64), pl.ds(64, 32)

    def shard(p, j, zr, r, half=None, rows=ALL, core=None):
        i1 = ALL if j is ALL else ring(mine1[p], j)
        iz = ALL if zr is ALL else ring(zl, zr)
        i2 = ring(mine2[p], r)
        yy, xx = (i2, i1) if p == 0 else (i1, i2)
        lanes = ALL if half is None else pl.ds(half * 128, 128)
        return bufs[p].at[yy, xx, iz, c if core is None else core, rows, lanes]

    def copy_of(key, src, dst, axis, s):
        return pltpu.make_async_remote_copy(
            src_ref=src,
            dst_ref=dst,
            send_sem=send_sem.at[SENT[key if key in GRADS else key[:2]]],
            recv_sem=recv_sem.at[RECV[key]],
            device_id=neighbour(axis, s),
            device_id_type=MESH,
        )

    def give(key, axis, s, *where, **also):
        ref = shard(*where, **also)
        copy_of(key, ref, ref, axis, s).start()

    def arrived(key, ref):
        copy_of(key, ref, ref, "core", 1).wait_recv()

    def taken(key, *where, **also):
        arrived(key, shard(*where, **also))

    def all_sent():
        for p in PARTS:
            b = bufs[p]
            for kind, ref in (
                ("t1", b.at[0, 0, 0]),
                ("t4", b.at[0, 0, 0, 0]),
                ("z1", b.at[0, 0]),
                ("g1", b.at[0, 0:3]),
                ("g2", b.at[0, 0:3, 0:2]),
                ("d1", b.at[0, 0]),
                ("d2", b.at[0, 0, 0:2]),
                ("c0", b.at[0, 0:2]),
                ("cg", b.at[0:3, 0:2, :, :, 0:64]),
                ("cd", b.at[0:3, 0:2, :, :, 64:96]),
            ):
                pltpu.make_async_remote_copy(
                    src_ref=ref,
                    dst_ref=ref,
                    send_sem=send_sem.at[SENT[kind, p]],
                    recv_sem=recv_sem.at[0],
                    device_id=neighbour("core", 1),
                    device_id_type=MESH,
                ).wait_send()

            def second(ref):
                copy_of(("z2", p), ref, ref, "core", 1).wait_send()

            @pl.when(jnp.logical_or(zg == 0, zg == 15))
            def _():
                second(b.at[0, 0, 0])

            @pl.when(jnp.logical_or(zg == 1, zg == 2))
            def _():
                second(b.at[0, 0:3, 0])

            @pl.when(jnp.logical_and(zg > 2, zg < 15))
            def _():
                second(b.at[0, 0, 0:2])

        for d in WAYS:
            for name, ref in (("rs1", rs1.at[d]), ("rs2", rs2.at[d]), ("ag1", mean_out.at[0]), ("ag2", mean_out.at[0, :, :, 0:128])):
                copy_of((name, d), ref, ref, "core", 1).wait_send()

    def tell(k, s):
        pl.semaphore_signal(here.at[k], inc=1, device_id=neighbour("z", s), device_id_type=MESH)

    def told(k):
        pl.semaphore_wait(here.at[k], 1)

    zg = h * 4 + zl

    loads = [
        pltpu.make_async_copy(src, dst, in_sem.at[k])
        for k, (src, dst) in enumerate(
            (
                (gain_hbm, gain_in),
                (gate_hbm, gate_in),
                (down_hbm, down_in),
                (up_hbm, up_in),
                (grads_hbm.at[0], grad_in),
                (tok_hbm, tok),
            )
        )
    ]
    for load in loads:
        load.start()

    barrier = pltpu.get_barrier_semaphore()
    partners = [("x", 1), ("x", -1), ("y", 1), ("y", -1), ("z", -1), ("core", 1)]
    for axis, s in partners:
        pl.semaphore_signal(barrier, inc=1, device_id=neighbour(axis, s), device_id_type=MESH)

    loads[0].wait()
    rows = lax.broadcasted_iota(jnp.int32, (64, 64), 0)
    cols = lax.broadcasted_iota(jnp.int32, (64, 64), 1)
    gain_row = jnp.broadcast_to(gain_in[...].astype(F32), (64, 64))
    gain = jnp.sum(jnp.where(rows == cols, gain_row, 0.0), axis=1, keepdims=True)
    loads[1].wait()
    buf_p[y, x, zl, c, 0:64, :] = (gate_in[...].astype(F32) * gain).astype(BF16)
    loads[2].wait()
    buf_p[y, x, zl, c, 64:96, :] = down_in[0:32]
    buf_q[y, x, zl, c, 64:96, :] = down_in[32:64]
    loads[3].wait()
    buf_q[y, x, zl, c, 0:64, :] = (up_in[...].astype(F32) * gain).astype(BF16)

    pl.semaphore_wait(barrier, len(partners))

    def quarter(ref, q, half=None):
        lanes = ALL if half is None else pl.ds(half * 128, 128)
        return ref.at[:, pl.ds(pl.multiple_of(q * 16, 16), 16), lanes]

    BOTH = [(p, d) for d in WAYS for p in PARTS]

    def along_z(p, j):
        give(("z1", p, 0, j), "z", 1, p, j, 0, 0)

        @pl.when(zg > 0)
        def _():
            give(("z1", p, 1, j), "z", -1, p, j, 0, 0)

    def along_last(p, zr, j):
        for e in WAYS:
            key = ("g1", p, e, zr, j) if zr == 0 else ("g1", p, e, zr)
            give(key, last[p], SIGN[e], p, j, zr, 0, rows=ALL if zr == 0 else GATED)

    for p, d in BOTH:
        give(("t1", p, d), first[p], SIGN[d], p, 0, 0, 0)
    tell(0, 1)
    for p in PARTS:
        give(("z1", p, 0, 0), "z", 1, p, 0, 0, 0)
    for p in PARTS:
        along_last(p, 0, 0)

    def below():
        told(0)
        tell(1, -1)
        tell(2, 1)

    def four_away():
        tell(3, -2)
        tell(4, 2)

    def exchange(d):
        src = quarter(grad_in, ring(h, 2), d)
        copy_of(("rs1", d), src, rs1.at[d], "cut", SIGN[d]).start()

    @pl.when(zg > 0)
    def _():
        below()
        for p in PARTS:
            give(("z1", p, 1, 0), "z", -1, p, 0, 0, 0)

    loads[4].wait()
    loads[5].wait()

    def square(k, total):
        v = tok[:, pl.ds(pl.multiple_of(k * 128, 128), 128)].astype(F32)
        return total + v * v

    total = lax.fori_loop(0, 64, square, jnp.zeros((128, 128), F32), unroll=4)
    mean = jnp.sum(total, axis=1, keepdims=True) * (1.0 / 8192.0)
    inv[...] = jnp.broadcast_to(lax.rsqrt(mean + 1e-5), (128, 128))
    acc[...] = jnp.zeros_like(acc)

    @pl.when(zg < 15)
    def _():
        told(1)

    @pl.when(zg > 1)
    def _():
        told(2)

    @pl.when(jnp.logical_and(zg > 1, zg < 15))
    def _():
        four_away()

    def first_axis(p, d):
        j = BACK[d]
        taken(("t1", p, d), p, j, 0, 0)
        give(("t4", p), first[p], SIGN[d], p, j, 0, 0, half=d)

    for p, d in BOTH:
        first_axis(p, d)

    @pl.when(zg == 15)
    def _():
        told(1)
        four_away()

    @pl.when(jnp.logical_and(zg > 7, zg < 13))
    def _():
        told(3)
        exchange(0)

    @pl.when(zg > 3)
    def _():
        told(4)
        exchange(1)

    for p, d in BOTH:
        along_z(p, BACK[d])
        along_last(p, 0, BACK[d])

    @pl.when(zg < 8)
    def _():
        told(3)
        exchange(0)

    def onward(p, d, j, half=True):
        give(("z2", p), "z", SIGN[d], p, j, BACK[d], 0, half=d if half else None)

    def from_z(d, js):
        zr = BACK[d]
        for j in js:
            for p in PARTS:
                taken(("z1", p, d, j), p, j, zr, 0)
                if d == 0:

                    @pl.when(jnp.logical_and(zg > 0, zg < 15))
                    def _():
                        onward(p, d, j)

                else:

                    @pl.when(zg > 2)
                    def _():
                        onward(p, d, j)

                    @pl.when(jnp.logical_or(zg == 1, zg == 2))
                    def _():
                        onward(p, d, j, half=False)

                along_last(p, zr, j)
        if js[-1] == 2:
            for p in PARTS:
                give(("c0", p), "core", 1, p, ALL, zr, 0)

    def first_far(p):
        taken(("t4", p), p, 2, 0, 0)
        along_z(p, 2)
        along_last(p, 0, 2)
        give(("c0", p), "core", 1, p, ALL, 0, 0)

    def down_near(zr):
        for p, d in BOTH:
            give(("d1", p, d, zr), last[p], SIGN[d], p, ALL, zr, 0, rows=DOWN)

    def gated_near(zr):
        for p, d in BOTH:
            r = BACK[d]
            taken(("g1", p, d, zr), p, ALL, zr, r, rows=GATED)
            give(("g2", p, zr), last[p], SIGN[d], p, ALL, zr, r, half=d, rows=GATED)
            give(("cg", p, r), "core", 1, p, ALL, zr, r, rows=GATED)

    def own_near(j):
        for p, d in BOTH:
            r = BACK[d]
            taken(("g1", p, d, 0, j), p, j, 0, r)
            give(("g2", p, 0), last[p], SIGN[d], p, j, 0, r, half=d)
            if j == 2:
                give(("cg", p, r), "core", 1, p, ALL, 0, r, rows=GATED)
                give(("cd", p, r), "core", 1, p, ALL, 0, r, rows=DOWN)

    def gated_far(zr):
        for p in PARTS:
            taken(("g2", p, zr), p, ALL, zr, 2, rows=ALL if zr == 0 else GATED)
            give(("cg", p, 2), "core", 1, p, ALL, zr, 2, rows=GATED)
            if zr == 0:
                give(("cd", p, 2), "core", 1, p, ALL, zr, 2, rows=DOWN)

    def down_next(zr):
        for p, d in BOTH:
            r = BACK[d]
            taken(("d1", p, d, zr), p, ALL, zr, r, rows=DOWN)
            give(("d2", p, zr), last[p], SIGN[d], p, ALL, zr, r, half=d, rows=DOWN)
            give(("cd", p, r), "core", 1, p, ALL, zr, r, rows=DOWN)

    def down_far(zr):
        for p in PARTS:
            taken(("d2", p, zr), p, ALL, zr, 2, rows=DOWN)
            give(("cd", p, 2), "core", 1, p, ALL, zr, 2, rows=DOWN)

    def across_z():
        for p in PARTS:
            taken(("z2", p), p, ALL, 2, 0)
            along_last(p, 2, ALL)
            give(("c0", p), "core", 1, p, ALL, 2, 0)

    def multiply(r):
        for p in PARTS:
            if r == 0:
                taken(("c0", p), p, ALL, ALL, 0, core=1 - c)
            else:
                taken(("cg", p, r), p, ALL, ALL, r, rows=GATED, core=1 - c)
            i2 = ring(mine2[p], r)
            n = pl.ds(p * 256, 256)
            total = acc[:, n]
            for k in range(4):
                yy, xx = (i2, k) if p == 0 else (k, i2)
                w = bufs[p][yy, xx, :, :, 0:64, :].reshape(512, 256)
                t = tok[:, pl.ds(pl.multiple_of((yy * 4 + xx) * 512, 512), 512)]
                total = total + jnp.dot(t, w, preferred_element_type=F32)
            acc[:, n] = total

    def grads_partial(d):
        arrived(("rs1", d), rs1.at[d])
        q = pl.ds(pl.multiple_of(ring(h, SIGN[d]) * 16, 16), 16)
        part[d] = grad_in[:, q, :]
        lanes = pl.ds(d * 128, 128)
        part[d, :, :, lanes] = grad_in[:, q, lanes] + rs1[d]

    def grads_send(d):
        copy_of(("rs2", d), part.at[d], rs2.at[d], "cut", SIGN[d]).start()

    def grads_own():
        q = pl.ds(pl.multiple_of(h * 16, 16), 16)
        for d in WAYS:
            arrived(("rs2", d), rs2.at[d])
        mean_out[h] = ((grad_in[:, q, :] + rs2[0] + rs2[1]) * 0.25).astype(BF16)

    def grads_give():
        for d in WAYS:
            copy_of(("ag1", d), mean_out.at[h], mean_out.at[h], "cut", SIGN[d]).start()

    def grads_next():
        for d in WAYS:
            arrived(("ag1", d), mean_out.at[ring(h, BACK[d])])
            half = mean_out.at[ring(h, BACK[d]), :, :, pl.ds(d * 128, 128)]
            copy_of(("ag2", d), half, half, "cut", SIGN[d]).start()

    own_near(0)

    @pl.when(zg > 12)
    def _():
        told(3)
        exchange(0)

    first_far(0)
    first_far(1)
    own_near(-1)
    own_near(1)

    @pl.when(zg < 15)
    def _():
        from_z(1, (0,))

    @pl.when(zg > 0)
    def _():
        from_z(0, (0,))

    @pl.when(zg == 0)
    def _():
        below()

    @pl.when(zg < 2)
    def _():
        told(2)
        four_away()

    @pl.when(jnp.logical_and(zg < 4, zg != 1))
    def _():
        told(4)
        exchange(1)

    @pl.when(zg == 0)
    def _():
        for p in PARTS:
            for j in NEAR:
                give(("z1", p, 1, j), "z", -1, p, j, 0, 0)
            onward(p, 1, 0)

    own_near(2)

    @pl.when(zg == 1)
    def _():
        told(4)
        exchange(1)

    @pl.when(zg > 11)
    def _():
        grads_partial(0)
        grads_send(0)

    @pl.when(zg == 15)
    def _():
        from_z(0, (-1, 1, 2))
        down_near(-1)
        grads_partial(1)
        grads_send(1)
        from_z(1, (0,))

    from_z(1, (-1, 1, 2))

    @pl.when(zg == 0)
    def _():
        for p in PARTS:
            for j in NEAR[1:]:
                onward(p, 1, j)

    down_near(1)

    @pl.when(jnp.logical_and(zg != 13, zg != 15))
    def _():
        grads_partial(1)
        grads_send(1)

    @pl.when(jnp.logical_or(zg == 0, jnp.logical_and(zg > 3, zg < 12)))
    def _():
        grads_partial(0)
        grads_send(0)

    @pl.when(zg == 0)
    def _():
        gated_near(1)
        down_next(1)
        from_z(0, (0,))

    @pl.when(zg < 15)
    def _():
        from_z(0, (-1, 1, 2))
        down_near(-1)

    @pl.when(zg == 13)
    def _():
        grads_partial(1)
        grads_send(1)


    @pl.when(zg > 0)
    def _():
        gated_near(1)
        down_next(1)

    @pl.when(jnp.logical_and(zg > 0, zg < 4))
    def _():
        grads_partial(0)
        grads_send(0)

    gated_near(-1)
    across_z()
    down_near(2)
    down_next(-1)
    grads_own()
    grads_give()
    gated_near(2)

    @pl.when(zg > 3)
    def _():
        grads_next()

    down_next(2)
    gated_far(0)
    gated_far(1)
    multiply(0)
    gated_far(-1)
    multiply(-1)
    gated_far(2)
    multiply(1)
    down_far(1)
    down_far(-1)
    multiply(2)

    gate = acc[:, 0:256] * inv[:, 0:1]
    up = acc[:, 256:512] * inv[:, 0:1]
    hid[...] = (gate / (1.0 + jnp.exp(-gate)) * up).astype(BF16)

    def project(yy, xx):
        w = jnp.concatenate([b[yy, xx, :, :, 64:96, :] for b in bufs], axis=2).reshape(512, 256)
        block = lax.dot_general(hid[...], w, (((1,), (1,)), ((), ())), preferred_element_type=F32)
        out[:, pl.ds(pl.multiple_of((yy * 4 + xx) * 512, 512), 512)] = block.astype(BF16)

    for p in PARTS:
        for r in (-1, 1):
            taken(("cd", p, r), p, ALL, ALL, r, rows=DOWN, core=1 - c)

    def near(k, _):
        for i in range(3):
            project(ring(y, k - 1), ring(x, i - 1))
        return 0

    def last_part():
        for p in PARTS:
            taken(("cd", p, 2), p, ALL, ALL, 2, rows=DOWN, core=1 - c)
        for k in range(4):
            project(ring(y, 2), k)
        for k in range(3):
            project(ring(y, k - 1), ring(x, 2))

    def finish():
        for d in WAYS:
            arrived(("ag2", d), mean_out.at[ring(h, 2), :, :, pl.ds(d * 128, 128)])
        for k in range(4):
            grad_out[:, k * 16 : k * 16 + 16, :] = mean_out[k].astype(F32)

    down_far(2)

    @pl.when(zg < 4)
    def _():
        grads_next()

    lax.fori_loop(0, 3, near, 0)
    finish()
    last_part()
    all_sent()


def per_device(tokens, norm_gain, gate_weight, up_weight, down_weight, slice_grads):
    hbm = pl.BlockSpec(memory_space=pltpu.HBM)
    vmem = pl.BlockSpec(memory_space=pltpu.VMEM)
    return pl.pallas_call(
        kernel,
        out_shape=(
            pltpu.VMEM(tokens.shape, BF16),
            pltpu.VMEM(slice_grads.shape[1:], F32),
        ),
        in_specs=[hbm] * 6,
        out_specs=(vmem, vmem),
        scratch_shapes=[
            pltpu.VMEM((4, 4, 4, 2, 96, 256), BF16),
            pltpu.VMEM((4, 4, 4, 2, 96, 256), BF16),
            pltpu.VMEM((128, 8192), BF16),
            pltpu.VMEM((128, 512), F32),
            pltpu.VMEM((128, 256), BF16),
            pltpu.VMEM((128, 128), F32),
            pltpu.VMEM((1, 64), BF16),
            pltpu.VMEM((64, 256), BF16),
            pltpu.VMEM((64, 256), BF16),
            pltpu.VMEM((64, 256), BF16),
            pltpu.VMEM((3, 64, 256), F32),
            pltpu.VMEM((2, 3, 16, 128), F32),
            pltpu.VMEM((2, 3, 16, 256), F32),
            pltpu.VMEM((2, 3, 16, 256), F32),
            pltpu.VMEM((4, 3, 16, 256), BF16),
            pltpu.SemaphoreType.DMA((len(SENT),)),
            pltpu.SemaphoreType.DMA((len(RECV),)),
            pltpu.SemaphoreType.DMA((6,)),
            pltpu.SemaphoreType.REGULAR((5,)),
        ],
        compiler_params=pltpu.CompilerParams(
            collective_id=0, has_side_effects=True, vmem_limit_bytes=60000000
        ),
    )(tokens, norm_gain.reshape(1, 64), gate_weight, up_weight, down_weight.T, slice_grads)


def solution(mesh):
    finer = Mesh(mesh.devices.reshape(mesh.shape["cuts"], 4, 4, 4, 2), CUTS_FSDP)
    in_specs = (
        P(CUTS_FSDP, None),
        P(FSDP),
        P(FSDP, None),
        P(FSDP, None),
        P(None, FSDP),
        P("cuts", None, FSDP, None),
    )
    out_specs = (P(CUTS_FSDP, None), P(None, FSDP, None))
    return jax.shard_map(
        per_device, mesh=finer, in_specs=in_specs, out_specs=out_specs, check_vma=False
    )
```

```python
import jax
import jax.numpy as jnp
from jax import lax
from jax.experimental import pallas as pl
from jax.experimental.pallas import tpu as pltpu
from jax.sharding import Mesh
from jax.sharding import PartitionSpec as P

MESH = pl.DeviceIdType.MESH
FSDP = ("y", "x", "zl", "core")
CUTS_FSDP = ("cuts", "y", "x", "zl", "core")
ALL = slice(None)
NEAR = (0, -1, 1, 2)
F32 = jnp.float32
BF16 = jnp.bfloat16


PARTS = range(2)
WAYS = range(2)

RECV = [("t1", p, d) for p in PARTS for d in WAYS]
RECV += [("t4", p) for p in PARTS] + [("z2", p) for p in PARTS] + [("c0", p) for p in PARTS]
RECV += [("z1", p, d, j) for p in PARTS for d in WAYS for j in NEAR]
RECV += [("g1", p, d, zr) for p in PARTS for d in WAYS for zr in NEAR[1:]]
RECV += [("g1", p, d, 0, j) for p in PARTS for d in WAYS for j in NEAR]
RECV += [("g2", p, zr) for p in PARTS for zr in NEAR]
RECV += [("d1", p, d, zr) for p in PARTS for d in WAYS for zr in NEAR[1:]]
RECV += [("d2", p, zr) for p in PARTS for zr in NEAR[1:]]
RECV += [(name, p, r) for name in ("cg", "cd") for p in PARTS for r in (-1, 1, 2)]
GRADS = [(name, d) for name in ("rs1", "rs2", "ag1", "ag2") for d in WAYS]
RECV = {key: k for k, key in enumerate(RECV + GRADS)}
KINDS = ("t1", "t4", "z1", "z2", "g1", "g2", "d1", "d2", "c0", "cg", "cd")
SENT = {key: k for k, key in enumerate([(kind, p) for kind in KINDS for p in PARTS] + GRADS)}


def kernel(
    tok_hbm, gain_hbm, gate_hbm, up_hbm, down_hbm, grads_hbm,
    out, mean_out,
    buf_p, buf_q, tok, acc, hid, inv,
    gain_in, gate_in, up_in, down_in,
    grad_in, rs1, part, rs2,
    send_sem, recv_sem, in_sem, here,
):
    bufs = (buf_p, buf_q)
    h, y, x, zl, c = (lax.axis_index(a) for a in CUTS_FSDP)

    def ring(v, s, n=4):
        return lax.rem(v + (s + n), n)

    def neighbour(axis, s):
        if axis == "y":
            return {"y": ring(y, s)}
        if axis == "x":
            return {"x": ring(x, s)}
        if axis == "cut":
            return {"cuts": ring(h, s)}
        if axis == "core":
            return {"core": 1 - c}
        zz = lax.rem(h * 4 + zl + (s + 16), 16)
        return {"cuts": lax.div(zz, 4), "zl": lax.rem(zz, 4)}

    SIGN = (1, -1)
    BACK = (-1, 1)
    first = ("x", "y")
    last = ("y", "x")
    mine1 = (x, y)
    mine2 = (y, x)

    GATED, DOWN = pl.ds(0, 64), pl.ds(64, 32)

    def shard(p, j, zr, r, half=None, rows=ALL, core=None):
        i1 = ALL if j is ALL else ring(mine1[p], j)
        iz = ALL if zr is ALL else ring(zl, zr)
        i2 = ring(mine2[p], r)
        yy, xx = (i2, i1) if p == 0 else (i1, i2)
        lanes = ALL if half is None else pl.ds(half * 128, 128)
        return bufs[p].at[yy, xx, iz, c if core is None else core, rows, lanes]

    def copy_of(key, src, dst, axis, s):
        return pltpu.make_async_remote_copy(
            src_ref=src,
            dst_ref=dst,
            send_sem=send_sem.at[SENT[key if key in GRADS else key[:2]]],
            recv_sem=recv_sem.at[RECV[key]],
            device_id=neighbour(axis, s),
            device_id_type=MESH,
        )

    def give(key, axis, s, *where, **also):
        ref = shard(*where, **also)
        copy_of(key, ref, ref, axis, s).start()

    def arrived(key, ref):
        copy_of(key, ref, ref, "core", 1).wait_recv()

    def taken(key, *where, **also):
        arrived(key, shard(*where, **also))

    def all_sent():
        for p in PARTS:
            b = bufs[p]
            for kind, ref in (
                ("t1", b.at[0, 0, 0]),
                ("t4", b.at[0, 0, 0, 0]),
                ("z1", b.at[0, 0]),
                ("g1", b.at[0, 0:3]),
                ("g2", b.at[0, 0:3, 0:2]),
                ("d1", b.at[0, 0]),
                ("d2", b.at[0, 0, 0:2]),
                ("c0", b.at[0, 0:2]),
                ("cg", b.at[0:3, 0:2, :, :, 0:64]),
                ("cd", b.at[0:3, 0:2, :, :, 64:96]),
            ):
                pltpu.make_async_remote_copy(
                    src_ref=ref,
                    dst_ref=ref,
                    send_sem=send_sem.at[SENT[kind, p]],
                    recv_sem=recv_sem.at[0],
                    device_id=neighbour("core", 1),
                    device_id_type=MESH,
                ).wait_send()

            def second(ref):
                copy_of(("z2", p), ref, ref, "core", 1).wait_send()

            @pl.when(jnp.logical_or(zg == 0, zg == 15))
            def _():
                second(b.at[0, 0, 0])

            @pl.when(jnp.logical_or(zg == 1, zg == 2))
            def _():
                second(b.at[0, 0:3, 0])

            @pl.when(jnp.logical_and(zg > 2, zg < 15))
            def _():
                second(b.at[0, 0, 0:2])

        for d in WAYS:
            for name, ref in (("rs1", rs1.at[d]), ("rs2", rs2.at[d]), ("ag1", mean_out.at[0]), ("ag2", mean_out.at[0, :, :, 0:128])):
                copy_of((name, d), ref, ref, "core", 1).wait_send()

    def tell(k, s):
        pl.semaphore_signal(here.at[k], inc=1, device_id=neighbour("z", s), device_id_type=MESH)

    def told(k):
        pl.semaphore_wait(here.at[k], 1)

    zg = h * 4 + zl

    loads = [
        pltpu.make_async_copy(src, dst, in_sem.at[k])
        for k, (src, dst) in enumerate(
            (
                (gain_hbm, gain_in),
                (gate_hbm, gate_in),
                (down_hbm, down_in),
                (up_hbm, up_in),
                (grads_hbm.at[0], grad_in),
                (tok_hbm, tok),
            )
        )
    ]
    for load in loads:
        load.start()

    barrier = pltpu.get_barrier_semaphore()
    partners = [("x", 1), ("x", -1), ("y", 1), ("y", -1), ("z", -1), ("core", 1)]
    for axis, s in partners:
        pl.semaphore_signal(barrier, inc=1, device_id=neighbour(axis, s), device_id_type=MESH)

    loads[0].wait()
    rows = lax.broadcasted_iota(jnp.int32, (64, 64), 0)
    cols = lax.broadcasted_iota(jnp.int32, (64, 64), 1)
    gain_row = jnp.broadcast_to(gain_in[...].astype(F32), (64, 64))
    gain = jnp.sum(jnp.where(rows == cols, gain_row, 0.0), axis=1, keepdims=True)
    loads[1].wait()
    buf_p[y, x, zl, c, 0:64, :] = (gate_in[...].astype(F32) * gain).astype(BF16)
    loads[2].wait()
    buf_p[y, x, zl, c, 64:96, :] = down_in[0:32]
    buf_q[y, x, zl, c, 64:96, :] = down_in[32:64]
    loads[3].wait()
    buf_q[y, x, zl, c, 0:64, :] = (up_in[...].astype(F32) * gain).astype(BF16)

    pl.semaphore_wait(barrier, len(partners))

    def quarter(ref, q, half=None):
        lanes = ALL if half is None else pl.ds(half * 128, 128)
        return ref.at[:, pl.ds(pl.multiple_of(q * 16, 16), 16), lanes]

    BOTH = [(p, d) for d in WAYS for p in PARTS]

    def along_z(p, j):
        give(("z1", p, 0, j), "z", 1, p, j, 0, 0)

        @pl.when(zg > 0)
        def _():
            give(("z1", p, 1, j), "z", -1, p, j, 0, 0)

    def along_last(p, zr, j):
        for e in WAYS:
            key = ("g1", p, e, zr, j) if zr == 0 else ("g1", p, e, zr)
            give(key, last[p], SIGN[e], p, j, zr, 0, rows=ALL if zr == 0 else GATED)

    for p, d in BOTH:
        give(("t1", p, d), first[p], SIGN[d], p, 0, 0, 0)
    tell(0, 1)
    for p in PARTS:
        give(("z1", p, 0, 0), "z", 1, p, 0, 0, 0)
    for p in PARTS:
        along_last(p, 0, 0)

    def below():
        told(0)
        tell(1, -1)
        tell(2, 1)

    def four_away():
        tell(3, -2)
        tell(4, 2)

    def exchange(d):
        src = quarter(grad_in, ring(h, 2), d)
        copy_of(("rs1", d), src, rs1.at[d], "cut", SIGN[d]).start()

    @pl.when(zg > 0)
    def _():
        below()
        for p in PARTS:
            give(("z1", p, 1, 0), "z", -1, p, 0, 0, 0)

    loads[4].wait()
    loads[5].wait()

    def square(k, total):
        v = tok[:, pl.ds(pl.multiple_of(k * 128, 128), 128)].astype(F32)
        return total + v * v

    total = lax.fori_loop(0, 64, square, jnp.zeros((128, 128), F32), unroll=4)
    mean = jnp.sum(total, axis=1, keepdims=True) * (1.0 / 8192.0)
    inv[...] = jnp.broadcast_to(lax.rsqrt(mean + 1e-5), (128, 128))
    acc[...] = jnp.zeros_like(acc)

    @pl.when(zg < 15)
    def _():
        told(1)

    @pl.when(zg > 1)
    def _():
        told(2)

    @pl.when(jnp.logical_and(zg > 1, zg < 15))
    def _():
        four_away()

    def first_axis(p, d):
        j = BACK[d]
        taken(("t1", p, d), p, j, 0, 0)
        give(("t4", p), first[p], SIGN[d], p, j, 0, 0, half=d)

    for p, d in BOTH:
        first_axis(p, d)

    @pl.when(zg == 15)
    def _():
        told(1)
        four_away()

    @pl.when(jnp.logical_and(zg > 7, zg < 13))
    def _():
        told(3)
        exchange(0)

    @pl.when(zg > 3)
    def _():
        told(4)
        exchange(1)

    for p, d in BOTH:
        along_z(p, BACK[d])
        along_last(p, 0, BACK[d])

    @pl.when(zg < 8)
    def _():
        told(3)
        exchange(0)

    def onward(p, d, j, half=True):
        give(("z2", p), "z", SIGN[d], p, j, BACK[d], 0, half=d if half else None)

    def from_z(d, js):
        zr = BACK[d]
        for j in js:
            for p in PARTS:
                taken(("z1", p, d, j), p, j, zr, 0)
                if d == 0:

                    @pl.when(jnp.logical_and(zg > 0, zg < 15))
                    def _():
                        onward(p, d, j)

                else:

                    @pl.when(zg > 2)
                    def _():
                        onward(p, d, j)

                    @pl.when(jnp.logical_or(zg == 1, zg == 2))
                    def _():
                        onward(p, d, j, half=False)

                along_last(p, zr, j)
        if js[-1] == 2:
            for p in PARTS:
                give(("c0", p), "core", 1, p, ALL, zr, 0)

    def first_far(p):
        taken(("t4", p), p, 2, 0, 0)
        along_z(p, 2)
        along_last(p, 0, 2)
        give(("c0", p), "core", 1, p, ALL, 0, 0)

    def down_near(zr):
        for p, d in BOTH:
            give(("d1", p, d, zr), last[p], SIGN[d], p, ALL, zr, 0, rows=DOWN)

    def gated_near(zr):
        for p, d in BOTH:
            r = BACK[d]
            taken(("g1", p, d, zr), p, ALL, zr, r, rows=GATED)
            give(("g2", p, zr), last[p], SIGN[d], p, ALL, zr, r, half=d, rows=GATED)
            give(("cg", p, r), "core", 1, p, ALL, zr, r, rows=GATED)

    def own_near(j):
        for p, d in BOTH:
            r = BACK[d]
            taken(("g1", p, d, 0, j), p, j, 0, r)
            give(("g2", p, 0), last[p], SIGN[d], p, j, 0, r, half=d)
            if j == 2:
                give(("cg", p, r), "core", 1, p, ALL, 0, r, rows=GATED)
                give(("cd", p, r), "core", 1, p, ALL, 0, r, rows=DOWN)

    def gated_far(zr):
        for p in PARTS:
            taken(("g2", p, zr), p, ALL, zr, 2, rows=ALL if zr == 0 else GATED)
            give(("cg", p, 2), "core", 1, p, ALL, zr, 2, rows=GATED)
            if zr == 0:
                give(("cd", p, 2), "core", 1, p, ALL, zr, 2, rows=DOWN)

    def down_next(zr):
        for p, d in BOTH:
            r = BACK[d]
            taken(("d1", p, d, zr), p, ALL, zr, r, rows=DOWN)
            give(("d2", p, zr), last[p], SIGN[d], p, ALL, zr, r, half=d, rows=DOWN)
            give(("cd", p, r), "core", 1, p, ALL, zr, r, rows=DOWN)

    def down_far(zr):
        for p in PARTS:
            taken(("d2", p, zr), p, ALL, zr, 2, rows=DOWN)
            give(("cd", p, 2), "core", 1, p, ALL, zr, 2, rows=DOWN)

    def across_z():
        for p in PARTS:
            taken(("z2", p), p, ALL, 2, 0)
            along_last(p, 2, ALL)
            give(("c0", p), "core", 1, p, ALL, 2, 0)

    def multiply(r):
        for p in PARTS:
            if r == 0:
                taken(("c0", p), p, ALL, ALL, 0, core=1 - c)
            else:
                taken(("cg", p, r), p, ALL, ALL, r, rows=GATED, core=1 - c)
            i2 = ring(mine2[p], r)
            n = pl.ds(p * 256, 256)
            total = acc[:, n]
            for k in range(4):
                yy, xx = (i2, k) if p == 0 else (k, i2)
                w = bufs[p][yy, xx, :, :, 0:64, :].reshape(512, 256)
                t = tok[:, pl.ds(pl.multiple_of((yy * 4 + xx) * 512, 512), 512)]
                total = total + jnp.dot(t, w, preferred_element_type=F32)
            acc[:, n] = total

    def grads_partial(d):
        arrived(("rs1", d), rs1.at[d])
        q = pl.ds(pl.multiple_of(ring(h, SIGN[d]) * 16, 16), 16)
        part[d] = grad_in[:, q, :]
        lanes = pl.ds(d * 128, 128)
        part[d, :, :, lanes] = grad_in[:, q, lanes] + rs1[d]

    def grads_send(d):
        copy_of(("rs2", d), part.at[d], rs2.at[d], "cut", SIGN[d]).start()

    def grads_own():
        q = pl.ds(pl.multiple_of(h * 16, 16), 16)
        for d in WAYS:
            arrived(("rs2", d), rs2.at[d])
        mean_out[h] = ((grad_in[:, q, :] + rs2[0] + rs2[1]) * 0.25).astype(BF16)

    def grads_give():
        for d in WAYS:
            copy_of(("ag1", d), mean_out.at[h], mean_out.at[h], "cut", SIGN[d]).start()

    def grads_next():
        for d in WAYS:
            arrived(("ag1", d), mean_out.at[ring(h, BACK[d])])
            half = mean_out.at[ring(h, BACK[d]), :, :, pl.ds(d * 128, 128)]
            copy_of(("ag2", d), half, half, "cut", SIGN[d]).start()

    own_near(0)

    @pl.when(zg > 12)
    def _():
        told(3)
        exchange(0)

    first_far(0)
    first_far(1)
    own_near(-1)
    own_near(1)

    @pl.when(zg < 15)
    def _():
        from_z(1, (0,))

    @pl.when(zg > 0)
    def _():
        from_z(0, (0,))

    @pl.when(zg == 0)
    def _():
        below()

    @pl.when(zg < 2)
    def _():
        told(2)
        four_away()

    @pl.when(jnp.logical_and(zg < 4, zg != 1))
    def _():
        told(4)
        exchange(1)

    @pl.when(zg == 0)
    def _():
        for p in PARTS:
            for j in NEAR:
                give(("z1", p, 1, j), "z", -1, p, j, 0, 0)
            onward(p, 1, 0)

    own_near(2)

    @pl.when(zg == 1)
    def _():
        told(4)
        exchange(1)

    @pl.when(zg > 11)
    def _():
        grads_partial(0)
        grads_send(0)

    @pl.when(zg == 15)
    def _():
        from_z(0, (-1, 1, 2))
        down_near(-1)
        grads_partial(1)
        grads_send(1)
        from_z(1, (0,))

    from_z(1, (-1, 1, 2))

    @pl.when(zg == 0)
    def _():
        for p in PARTS:
            for j in NEAR[1:]:
                onward(p, 1, j)

    down_near(1)

    @pl.when(jnp.logical_and(zg != 13, zg != 15))
    def _():
        grads_partial(1)
        grads_send(1)

    @pl.when(jnp.logical_or(zg == 0, jnp.logical_and(zg > 3, zg < 12)))
    def _():
        grads_partial(0)
        grads_send(0)

    @pl.when(zg == 0)
    def _():
        gated_near(1)
        down_next(1)
        from_z(0, (0,))

    @pl.when(zg < 15)
    def _():
        from_z(0, (-1, 1, 2))
        down_near(-1)

    @pl.when(zg == 13)
    def _():
        grads_partial(1)
        grads_send(1)


    @pl.when(zg > 0)
    def _():
        gated_near(1)
        down_next(1)

    @pl.when(jnp.logical_and(zg > 0, zg < 4))
    def _():
        grads_partial(0)
        grads_send(0)

    gated_near(-1)
    across_z()
    down_near(2)
    grads_own()
    grads_give()
    down_next(-1)
    @pl.when(zg > 11)
    def _():
        grads_next()

    gated_near(2)

    @pl.when(jnp.logical_and(zg > 3, zg < 12))
    def _():
        grads_next()

    down_next(2)
    gated_far(0)
    gated_far(1)
    multiply(0)
    gated_far(-1)
    multiply(-1)
    gated_far(2)
    multiply(1)
    down_far(1)
    down_far(-1)
    multiply(2)

    gate = acc[:, 0:256] * inv[:, 0:1]
    up = acc[:, 256:512] * inv[:, 0:1]
    hid[...] = (gate / (1.0 + jnp.exp(-gate)) * up).astype(BF16)

    def project(yy, xx):
        w = jnp.concatenate([b[yy, xx, :, :, 64:96, :] for b in bufs], axis=2).reshape(512, 256)
        block = lax.dot_general(hid[...], w, (((1,), (1,)), ((), ())), preferred_element_type=F32)
        out[:, pl.ds(pl.multiple_of((yy * 4 + xx) * 512, 512), 512)] = block.astype(BF16)

    for p in PARTS:
        for r in (-1, 1):
            taken(("cd", p, r), p, ALL, ALL, r, rows=DOWN, core=1 - c)

    def near(k, _):
        for i in range(3):
            project(ring(y, k - 1), ring(x, i - 1))
        return 0

    def last_part():
        for p in PARTS:
            taken(("cd", p, 2), p, ALL, ALL, 2, rows=DOWN, core=1 - c)
        for k in range(4):
            project(ring(y, 2), k)
        for k in range(3):
            project(ring(y, k - 1), ring(x, 2))

    def finish():
        for d in WAYS:
            arrived(("ag2", d), mean_out.at[ring(h, 2), :, :, pl.ds(d * 128, 128)])

    down_far(2)

    @pl.when(zg < 4)
    def _():
        grads_next()

    lax.fori_loop(0, 3, near, 0)
    last_part()
    finish()
    all_sent()


def write_out(branch, means, out_hbm, grad_hbm, grads, sems):
    chunk = branch.shape[1] // 4
    stores = [
        pltpu.make_async_copy(
            branch.at[:, k * chunk : (k + 1) * chunk],
            out_hbm.at[:, k * chunk : (k + 1) * chunk],
            sems.at[k],
        )
        for k in range(4)
    ]
    for store in stores:
        store.start()
    for k in range(4):
        grads[:, k * 16 : k * 16 + 16, :] = means[k].astype(F32)
    stores.append(pltpu.make_async_copy(grads, grad_hbm, sems.at[4]))
    stores[4].start()
    for store in stores:
        store.wait()


def per_device(tokens, norm_gain, gate_weight, up_weight, down_weight, slice_grads):
    hbm = pl.BlockSpec(memory_space=pltpu.HBM)
    vmem = pl.BlockSpec(memory_space=pltpu.VMEM)
    branch, means = pl.pallas_call(
        kernel,
        out_shape=(
            pltpu.VMEM(tokens.shape, BF16),
            pltpu.VMEM((4, 3, 16, 256), BF16),
        ),
        in_specs=[hbm] * 6,
        out_specs=(vmem, vmem),
        scratch_shapes=[
            pltpu.VMEM((4, 4, 4, 2, 96, 256), BF16),
            pltpu.VMEM((4, 4, 4, 2, 96, 256), BF16),
            pltpu.VMEM((128, 8192), BF16),
            pltpu.VMEM((128, 512), F32),
            pltpu.VMEM((128, 256), BF16),
            pltpu.VMEM((128, 128), F32),
            pltpu.VMEM((1, 64), BF16),
            pltpu.VMEM((64, 256), BF16),
            pltpu.VMEM((64, 256), BF16),
            pltpu.VMEM((64, 256), BF16),
            pltpu.VMEM((3, 64, 256), F32),
            pltpu.VMEM((2, 3, 16, 128), F32),
            pltpu.VMEM((2, 3, 16, 256), F32),
            pltpu.VMEM((2, 3, 16, 256), F32),
            pltpu.SemaphoreType.DMA((len(SENT),)),
            pltpu.SemaphoreType.DMA((len(RECV),)),
            pltpu.SemaphoreType.DMA((6,)),
            pltpu.SemaphoreType.REGULAR((5,)),
        ],
        compiler_params=pltpu.CompilerParams(
            collective_id=0, has_side_effects=True, vmem_limit_bytes=60000000
        ),
    )(tokens, norm_gain.reshape(1, 64), gate_weight, up_weight, down_weight.T, slice_grads)
    return pl.pallas_call(
        write_out,
        out_shape=(
            pltpu.HBM(tokens.shape, BF16),
            pltpu.HBM(slice_grads.shape[1:], F32),
        ),
        in_specs=[vmem, vmem],
        out_specs=(hbm, hbm),
        scratch_shapes=[
            pltpu.VMEM(slice_grads.shape[1:], F32),
            pltpu.SemaphoreType.DMA((5,)),
        ],
        compiler_params=pltpu.CompilerParams(vmem_limit_bytes=8 * 1024 * 1024),
    )(branch, means)


def solution(mesh):
    finer = Mesh(mesh.devices.reshape(mesh.shape["cuts"], 4, 4, 4, 2), CUTS_FSDP)
    in_specs = (
        P(CUTS_FSDP, None),
        P(FSDP),
        P(FSDP, None),
        P(FSDP, None),
        P(None, FSDP),
        P("cuts", None, FSDP, None),
    )
    out_specs = (P(CUTS_FSDP, None), P(None, FSDP, None))
    return jax.shard_map(
        per_device, mesh=finer, in_specs=in_specs, out_specs=out_specs, check_vma=False
    )
```

```python
import jax
import jax.numpy as jnp
from jax import lax
from jax.experimental import pallas as pl
from jax.experimental.pallas import tpu as pltpu
from jax.sharding import Mesh
from jax.sharding import PartitionSpec as P

MESH = pl.DeviceIdType.MESH
FSDP = ("y", "x", "zl", "core")
CUTS_FSDP = ("cuts", "y", "x", "zl", "core")
ALL = slice(None)
NEAR = (0, -1, 1, 2)
F32 = jnp.float32
BF16 = jnp.bfloat16


PARTS = range(2)
WAYS = range(2)

RECV = [("t1", p, d) for p in PARTS for d in WAYS]
RECV += [("t4", p) for p in PARTS] + [("z2", p) for p in PARTS] + [("c0", p) for p in PARTS]
RECV += [("z1", p, d, j) for p in PARTS for d in WAYS for j in NEAR]
RECV += [("g1", p, d, zr) for p in PARTS for d in WAYS for zr in NEAR[1:]]
RECV += [("g1", p, d, 0, j) for p in PARTS for d in WAYS for j in NEAR]
RECV += [("g2", p, zr) for p in PARTS for zr in NEAR]
RECV += [("d1", p, d, zr) for p in PARTS for d in WAYS for zr in NEAR[1:]]
RECV += [("d2", p, zr) for p in PARTS for zr in NEAR[1:]]
RECV += [(name, p, r) for name in ("cg", "cd") for p in PARTS for r in (-1, 1, 2)]
GRADS = [(name, d) for name in ("rs1", "rs2", "ag1", "ag2") for d in WAYS]
RECV = {key: k for k, key in enumerate(RECV + GRADS)}
KINDS = ("t1", "t4", "z1", "z2", "g1", "g2", "d1", "d2", "c0", "cg", "cd")
SENT = {key: k for k, key in enumerate([(kind, p) for kind in KINDS for p in PARTS] + GRADS)}


def kernel(
    tok_hbm, gain_hbm, gate_hbm, up_hbm, down_hbm, grads_hbm,
    out, mean_out,
    buf_p, buf_q, tok, acc, hid, inv,
    gain_in, gate_in, up_in, down_in,
    grad_in, rs1, part, rs2,
    send_sem, recv_sem, in_sem, here,
):
    bufs = (buf_p, buf_q)
    h, y, x, zl, c = (lax.axis_index(a) for a in CUTS_FSDP)

    def ring(v, s, n=4):
        return lax.rem(v + (s + n), n)

    def neighbour(axis, s):
        if axis == "y":
            return {"y": ring(y, s)}
        if axis == "x":
            return {"x": ring(x, s)}
        if axis == "cut":
            return {"cuts": ring(h, s)}
        if axis == "core":
            return {"core": 1 - c}
        zz = lax.rem(h * 4 + zl + (s + 16), 16)
        return {"cuts": lax.div(zz, 4), "zl": lax.rem(zz, 4)}

    SIGN = (1, -1)
    BACK = (-1, 1)
    first = ("x", "y")
    last = ("y", "x")
    mine1 = (x, y)
    mine2 = (y, x)

    GATED, DOWN = pl.ds(0, 64), pl.ds(64, 32)

    def shard(p, j, zr, r, half=None, rows=ALL, core=None):
        i1 = ALL if j is ALL else ring(mine1[p], j)
        iz = ALL if zr is ALL else ring(zl, zr)
        i2 = ring(mine2[p], r)
        yy, xx = (i2, i1) if p == 0 else (i1, i2)
        lanes = ALL if half is None else pl.ds(half * 128, 128)
        return bufs[p].at[yy, xx, iz, c if core is None else core, rows, lanes]

    def copy_of(key, src, dst, axis, s):
        return pltpu.make_async_remote_copy(
            src_ref=src,
            dst_ref=dst,
            send_sem=send_sem.at[SENT[key if key in GRADS else key[:2]]],
            recv_sem=recv_sem.at[RECV[key]],
            device_id=neighbour(axis, s),
            device_id_type=MESH,
        )

    def give(key, axis, s, *where, **also):
        ref = shard(*where, **also)
        copy_of(key, ref, ref, axis, s).start()

    def arrived(key, ref):
        copy_of(key, ref, ref, "core", 1).wait_recv()

    def taken(key, *where, **also):
        arrived(key, shard(*where, **also))

    def all_sent():
        for p in PARTS:
            b = bufs[p]
            for kind, ref in (
                ("t1", b.at[0, 0, 0]),
                ("t4", b.at[0, 0, 0, 0]),
                ("z1", b.at[0, 0]),
                ("g1", b.at[0, 0:3]),
                ("g2", b.at[0, 0:3, 0:2]),
                ("d1", b.at[0, 0]),
                ("d2", b.at[0, 0, 0:2]),
                ("c0", b.at[0, 0:2]),
                ("cg", b.at[0:3, 0:2, :, :, 0:64]),
                ("cd", b.at[0:3, 0:2, :, :, 64:96]),
            ):
                pltpu.make_async_remote_copy(
                    src_ref=ref,
                    dst_ref=ref,
                    send_sem=send_sem.at[SENT[kind, p]],
                    recv_sem=recv_sem.at[0],
                    device_id=neighbour("core", 1),
                    device_id_type=MESH,
                ).wait_send()

            def second(ref):
                copy_of(("z2", p), ref, ref, "core", 1).wait_send()

            @pl.when(jnp.logical_or(zg == 0, zg == 15))
            def _():
                second(b.at[0, 0, 0])

            @pl.when(jnp.logical_or(zg == 1, zg == 2))
            def _():
                second(b.at[0, 0:3, 0])

            @pl.when(jnp.logical_and(zg > 2, zg < 15))
            def _():
                second(b.at[0, 0, 0:2])

        for d in WAYS:
            for name, ref in (("rs1", rs1.at[d]), ("rs2", rs2.at[d]), ("ag1", mean_out.at[0]), ("ag2", mean_out.at[0, :, :, 0:128])):
                copy_of((name, d), ref, ref, "core", 1).wait_send()

    def tell(k, s):
        pl.semaphore_signal(here.at[k], inc=1, device_id=neighbour("z", s), device_id_type=MESH)

    def told(k):
        pl.semaphore_wait(here.at[k], 1)

    zg = h * 4 + zl

    loads = [
        pltpu.make_async_copy(src, dst, in_sem.at[k])
        for k, (src, dst) in enumerate(
            (
                (gain_hbm, gain_in),
                (gate_hbm, gate_in),
                (down_hbm, down_in),
                (up_hbm, up_in),
                (grads_hbm.at[0], grad_in),
                (tok_hbm, tok),
            )
        )
    ]
    for load in loads:
        load.start()

    barrier = pltpu.get_barrier_semaphore()
    partners = [("x", 1), ("x", -1), ("y", 1), ("y", -1), ("z", -1), ("core", 1)]
    for axis, s in partners:
        pl.semaphore_signal(barrier, inc=1, device_id=neighbour(axis, s), device_id_type=MESH)

    loads[0].wait()
    rows = lax.broadcasted_iota(jnp.int32, (64, 64), 0)
    cols = lax.broadcasted_iota(jnp.int32, (64, 64), 1)
    gain_row = jnp.broadcast_to(gain_in[...].astype(F32), (64, 64))
    gain = jnp.sum(jnp.where(rows == cols, gain_row, 0.0), axis=1, keepdims=True)
    loads[1].wait()
    buf_p[y, x, zl, c, 0:64, :] = (gate_in[...].astype(F32) * gain).astype(BF16)
    loads[2].wait()
    buf_p[y, x, zl, c, 64:96, :] = down_in[0:32]
    buf_q[y, x, zl, c, 64:96, :] = down_in[32:64]
    loads[3].wait()
    buf_q[y, x, zl, c, 0:64, :] = (up_in[...].astype(F32) * gain).astype(BF16)

    pl.semaphore_wait(barrier, len(partners))

    def quarter(ref, q, half=None):
        lanes = ALL if half is None else pl.ds(half * 128, 128)
        return ref.at[:, pl.ds(pl.multiple_of(q * 16, 16), 16), lanes]

    BOTH = [(p, d) for d in WAYS for p in PARTS]

    def along_z(p, j):
        give(("z1", p, 0, j), "z", 1, p, j, 0, 0)

        @pl.when(zg > 0)
        def _():
            give(("z1", p, 1, j), "z", -1, p, j, 0, 0)

    def along_last(p, zr, j):
        for e in WAYS:
            key = ("g1", p, e, zr, j) if zr == 0 else ("g1", p, e, zr)
            give(key, last[p], SIGN[e], p, j, zr, 0, rows=ALL if zr == 0 else GATED)

    for p, d in BOTH:
        give(("t1", p, d), first[p], SIGN[d], p, 0, 0, 0)
    tell(0, 1)
    for p in PARTS:
        give(("z1", p, 0, 0), "z", 1, p, 0, 0, 0)
    for p in PARTS:
        along_last(p, 0, 0)

    def below():
        told(0)
        tell(1, -1)
        tell(2, 1)

    def four_away():
        tell(3, -2)
        tell(4, 2)

    def exchange(d):
        src = quarter(grad_in, ring(h, 2), d)
        copy_of(("rs1", d), src, rs1.at[d], "cut", SIGN[d]).start()

    @pl.when(zg > 0)
    def _():
        below()
        for p in PARTS:
            give(("z1", p, 1, 0), "z", -1, p, 0, 0, 0)

    loads[4].wait()
    loads[5].wait()

    def square(k, total):
        v = tok[:, pl.ds(pl.multiple_of(k * 128, 128), 128)].astype(F32)
        return total + v * v

    total = lax.fori_loop(0, 64, square, jnp.zeros((128, 128), F32), unroll=4)
    mean = jnp.sum(total, axis=1, keepdims=True) * (1.0 / 8192.0)
    inv[...] = jnp.broadcast_to(lax.rsqrt(mean + 1e-5), (128, 128))
    acc[...] = jnp.zeros_like(acc)

    @pl.when(zg < 15)
    def _():
        told(1)

    @pl.when(zg > 1)
    def _():
        told(2)

    @pl.when(jnp.logical_and(zg > 1, zg < 15))
    def _():
        four_away()

    def first_axis(p, d):
        j = BACK[d]
        taken(("t1", p, d), p, j, 0, 0)
        give(("t4", p), first[p], SIGN[d], p, j, 0, 0, half=d)

    for p, d in BOTH:
        first_axis(p, d)

    @pl.when(zg == 15)
    def _():
        told(1)
        four_away()

    @pl.when(jnp.logical_and(zg > 7, zg < 13))
    def _():
        told(3)
        exchange(0)

    @pl.when(zg > 3)
    def _():
        told(4)
        exchange(1)

    for p, d in BOTH:
        along_z(p, BACK[d])
        along_last(p, 0, BACK[d])

    @pl.when(zg < 8)
    def _():
        told(3)
        exchange(0)

    def onward(p, d, j, half=True):
        give(("z2", p), "z", SIGN[d], p, j, BACK[d], 0, half=d if half else None)

    def from_z(d, js):
        zr = BACK[d]
        for j in js:
            for p in PARTS:
                taken(("z1", p, d, j), p, j, zr, 0)
                if d == 0:

                    @pl.when(jnp.logical_and(zg > 0, zg < 15))
                    def _():
                        onward(p, d, j)

                else:

                    @pl.when(zg > 2)
                    def _():
                        onward(p, d, j)

                    @pl.when(jnp.logical_or(zg == 1, zg == 2))
                    def _():
                        onward(p, d, j, half=False)

                along_last(p, zr, j)
        if js[-1] == 2:
            for p in PARTS:
                give(("c0", p), "core", 1, p, ALL, zr, 0)

    def first_far(p):
        taken(("t4", p), p, 2, 0, 0)
        along_z(p, 2)
        along_last(p, 0, 2)
        give(("c0", p), "core", 1, p, ALL, 0, 0)

    def down_near(zr):
        for p, d in BOTH:
            give(("d1", p, d, zr), last[p], SIGN[d], p, ALL, zr, 0, rows=DOWN)

    def gated_near(zr):
        for p, d in BOTH:
            r = BACK[d]
            taken(("g1", p, d, zr), p, ALL, zr, r, rows=GATED)
            give(("g2", p, zr), last[p], SIGN[d], p, ALL, zr, r, half=d, rows=GATED)
            give(("cg", p, r), "core", 1, p, ALL, zr, r, rows=GATED)

    def own_near(j):
        for p, d in BOTH:
            r = BACK[d]
            taken(("g1", p, d, 0, j), p, j, 0, r)
            give(("g2", p, 0), last[p], SIGN[d], p, j, 0, r, half=d)
            if j == 2:
                give(("cg", p, r), "core", 1, p, ALL, 0, r, rows=GATED)
                give(("cd", p, r), "core", 1, p, ALL, 0, r, rows=DOWN)

    def gated_far(zr):
        for p in PARTS:
            taken(("g2", p, zr), p, ALL, zr, 2, rows=ALL if zr == 0 else GATED)
            give(("cg", p, 2), "core", 1, p, ALL, zr, 2, rows=GATED)
            if zr == 0:
                give(("cd", p, 2), "core", 1, p, ALL, zr, 2, rows=DOWN)

    def down_next(zr):
        for p, d in BOTH:
            r = BACK[d]
            taken(("d1", p, d, zr), p, ALL, zr, r, rows=DOWN)
            give(("d2", p, zr), last[p], SIGN[d], p, ALL, zr, r, half=d, rows=DOWN)
            give(("cd", p, r), "core", 1, p, ALL, zr, r, rows=DOWN)

    def down_far(zr):
        for p in PARTS:
            taken(("d2", p, zr), p, ALL, zr, 2, rows=DOWN)
            give(("cd", p, 2), "core", 1, p, ALL, zr, 2, rows=DOWN)

    def across_z():
        for p in PARTS:
            taken(("z2", p), p, ALL, 2, 0)
            along_last(p, 2, ALL)
            give(("c0", p), "core", 1, p, ALL, 2, 0)

    def multiply(r):
        for p in PARTS:
            if r == 0:
                taken(("c0", p), p, ALL, ALL, 0, core=1 - c)
            else:
                taken(("cg", p, r), p, ALL, ALL, r, rows=GATED, core=1 - c)
            i2 = ring(mine2[p], r)
            n = pl.ds(p * 256, 256)
            total = acc[:, n]
            for k in range(4):
                yy, xx = (i2, k) if p == 0 else (k, i2)
                w = bufs[p][yy, xx, :, :, 0:64, :].reshape(512, 256)
                t = tok[:, pl.ds(pl.multiple_of((yy * 4 + xx) * 512, 512), 512)]
                total = total + jnp.dot(t, w, preferred_element_type=F32)
            acc[:, n] = total

    def grads_partial(d):
        arrived(("rs1", d), rs1.at[d])
        q = pl.ds(pl.multiple_of(ring(h, SIGN[d]) * 16, 16), 16)
        part[d] = grad_in[:, q, :]
        lanes = pl.ds(d * 128, 128)
        part[d, :, :, lanes] = grad_in[:, q, lanes] + rs1[d]

    def grads_send(d):
        copy_of(("rs2", d), part.at[d], rs2.at[d], "cut", SIGN[d]).start()

    def grads_own():
        q = pl.ds(pl.multiple_of(h * 16, 16), 16)
        for d in WAYS:
            arrived(("rs2", d), rs2.at[d])
        mean_out[h] = ((grad_in[:, q, :] + rs2[0] + rs2[1]) * 0.25).astype(BF16)

    def grads_give():
        for d in WAYS:
            copy_of(("ag1", d), mean_out.at[h], mean_out.at[h], "cut", SIGN[d]).start()

    def grads_next():
        for d in WAYS:
            arrived(("ag1", d), mean_out.at[ring(h, BACK[d])])
            half = mean_out.at[ring(h, BACK[d]), :, :, pl.ds(d * 128, 128)]
            copy_of(("ag2", d), half, half, "cut", SIGN[d]).start()

    own_near(0)

    @pl.when(zg > 12)
    def _():
        told(3)
        exchange(0)

    first_far(0)
    first_far(1)
    own_near(-1)
    own_near(1)

    @pl.when(zg < 15)
    def _():
        from_z(1, (0,))

    @pl.when(zg > 0)
    def _():
        from_z(0, (0,))

    @pl.when(zg == 0)
    def _():
        below()

    @pl.when(zg < 2)
    def _():
        told(2)
        four_away()

    @pl.when(jnp.logical_and(zg < 4, zg != 1))
    def _():
        told(4)
        exchange(1)

    @pl.when(zg == 0)
    def _():
        for p in PARTS:
            for j in NEAR:
                give(("z1", p, 1, j), "z", -1, p, j, 0, 0)
            onward(p, 1, 0)

    own_near(2)

    @pl.when(zg == 1)
    def _():
        told(4)
        exchange(1)

    @pl.when(zg > 11)
    def _():
        grads_partial(0)
        grads_send(0)

    @pl.when(zg == 15)
    def _():
        from_z(0, (-1, 1, 2))
        down_near(-1)
        grads_partial(1)
        grads_send(1)
        from_z(1, (0,))

    from_z(1, (-1, 1, 2))

    @pl.when(zg == 0)
    def _():
        for p in PARTS:
            for j in NEAR[1:]:
                onward(p, 1, j)

    down_near(1)

    @pl.when(jnp.logical_and(zg != 13, zg != 15))
    def _():
        grads_partial(1)
        grads_send(1)

    @pl.when(jnp.logical_or(zg == 0, jnp.logical_and(zg > 3, zg < 12)))
    def _():
        grads_partial(0)
        grads_send(0)

    @pl.when(zg == 0)
    def _():
        gated_near(1)
        down_next(1)
        from_z(0, (0,))

    @pl.when(zg < 15)
    def _():
        from_z(0, (-1, 1, 2))
        down_near(-1)

    @pl.when(zg == 13)
    def _():
        grads_partial(1)
        grads_send(1)


    @pl.when(zg > 0)
    def _():
        gated_near(1)
        down_next(1)

    @pl.when(jnp.logical_and(zg > 0, zg < 4))
    def _():
        grads_partial(0)
        grads_send(0)

    gated_near(-1)
    across_z()
    down_near(2)
    grads_own()
    grads_give()
    down_next(-1)
    @pl.when(zg > 11)
    def _():
        grads_next()

    gated_near(2)

    @pl.when(jnp.logical_and(zg > 3, zg < 12))
    def _():
        grads_next()

    down_next(2)
    gated_far(0)
    gated_far(1)

    @pl.when(c == 1)
    def _():
        gated_far(-1)
        gated_far(2)

    multiply(0)

    @pl.when(c == 0)
    def _():
        gated_far(-1)

    multiply(-1)
    multiply(1)

    @pl.when(c == 0)
    def _():
        gated_far(2)

    down_far(1)
    down_far(-1)
    multiply(2)

    gate = acc[:, 0:256] * inv[:, 0:1]
    up = acc[:, 256:512] * inv[:, 0:1]
    hid[...] = (gate / (1.0 + jnp.exp(-gate)) * up).astype(BF16)

    def project(yy, xx):
        w = jnp.concatenate([b[yy, xx, :, :, 64:96, :] for b in bufs], axis=2).reshape(512, 256)
        block = lax.dot_general(hid[...], w, (((1,), (1,)), ((), ())), preferred_element_type=F32)
        out[:, pl.ds(pl.multiple_of((yy * 4 + xx) * 512, 512), 512)] = block.astype(BF16)

    for p in PARTS:
        for r in (-1, 1):
            taken(("cd", p, r), p, ALL, ALL, r, rows=DOWN, core=1 - c)

    def near(k, _):
        for i in range(3):
            project(ring(y, k - 1), ring(x, i - 1))
        return 0

    def last_part():
        for p in PARTS:
            taken(("cd", p, 2), p, ALL, ALL, 2, rows=DOWN, core=1 - c)
        for k in range(4):
            project(ring(y, 2), k)
        for k in range(3):
            project(ring(y, k - 1), ring(x, 2))

    def finish():
        for d in WAYS:
            arrived(("ag2", d), mean_out.at[ring(h, 2), :, :, pl.ds(d * 128, 128)])

    down_far(2)

    @pl.when(zg < 4)
    def _():
        grads_next()

    for k in range(3):
        near(k, 0)
    last_part()
    finish()
    all_sent()


def write_out(branch, means, out_hbm, grad_hbm, grads, sems):
    chunk = branch.shape[1] // 4
    stores = [
        pltpu.make_async_copy(
            branch.at[:, k * chunk : (k + 1) * chunk],
            out_hbm.at[:, k * chunk : (k + 1) * chunk],
            sems.at[k],
        )
        for k in range(4)
    ]
    for k, store in enumerate(stores):
        store.start(priority=k % 2)
    for k in range(4):
        grads[:, k * 16 : k * 16 + 16, :] = means[k].astype(F32)
    stores.append(pltpu.make_async_copy(grads, grad_hbm, sems.at[4]))
    stores[4].start()
    for store in stores:
        store.wait()


def per_device(tokens, norm_gain, gate_weight, up_weight, down_weight, slice_grads):
    hbm = pl.BlockSpec(memory_space=pltpu.HBM)
    vmem = pl.BlockSpec(memory_space=pltpu.VMEM)
    branch, means = pl.pallas_call(
        kernel,
        out_shape=(
            pltpu.VMEM(tokens.shape, BF16),
            pltpu.VMEM((4, 3, 16, 256), BF16),
        ),
        in_specs=[hbm] * 6,
        out_specs=(vmem, vmem),
        scratch_shapes=[
            pltpu.VMEM((4, 4, 4, 2, 96, 256), BF16),
            pltpu.VMEM((4, 4, 4, 2, 96, 256), BF16),
            pltpu.VMEM((128, 8192), BF16),
            pltpu.VMEM((128, 512), F32),
            pltpu.VMEM((128, 256), BF16),
            pltpu.VMEM((128, 128), F32),
            pltpu.VMEM((1, 64), BF16),
            pltpu.VMEM((64, 256), BF16),
            pltpu.VMEM((64, 256), BF16),
            pltpu.VMEM((64, 256), BF16),
            pltpu.VMEM((3, 64, 256), F32),
            pltpu.VMEM((2, 3, 16, 128), F32),
            pltpu.VMEM((2, 3, 16, 256), F32),
            pltpu.VMEM((2, 3, 16, 256), F32),
            pltpu.SemaphoreType.DMA((len(SENT),)),
            pltpu.SemaphoreType.DMA((len(RECV),)),
            pltpu.SemaphoreType.DMA((6,)),
            pltpu.SemaphoreType.REGULAR((5,)),
        ],
        compiler_params=pltpu.CompilerParams(
            collective_id=0, has_side_effects=True, vmem_limit_bytes=60000000
        ),
    )(tokens, norm_gain.reshape(1, 64), gate_weight, up_weight, down_weight.T, slice_grads)
    return pl.pallas_call(
        write_out,
        out_shape=(
            pltpu.HBM(tokens.shape, BF16),
            pltpu.HBM(slice_grads.shape[1:], F32),
        ),
        in_specs=[vmem, vmem],
        out_specs=(hbm, hbm),
        scratch_shapes=[
            pltpu.VMEM(slice_grads.shape[1:], F32),
            pltpu.SemaphoreType.DMA((5,)),
        ],
        compiler_params=pltpu.CompilerParams(vmem_limit_bytes=8 * 1024 * 1024),
    )(branch, means)


def solution(mesh):
    finer = Mesh(mesh.devices.reshape(mesh.shape["cuts"], 4, 4, 4, 2), CUTS_FSDP)
    in_specs = (
        P(CUTS_FSDP, None),
        P(FSDP),
        P(FSDP, None),
        P(FSDP, None),
        P(None, FSDP),
        P("cuts", None, FSDP, None),
    )
    out_specs = (P(CUTS_FSDP, None), P(None, FSDP, None))
    return jax.shard_map(
        per_device, mesh=finer, in_specs=in_specs, out_specs=out_specs, check_vma=False
    )
```
